32 devices in a mesh: tm: 32 (over z, y, x, core), panel: 1.
Axes of the slice: x: 2, y: 2, z: 4, core: 2. Of those that a mesh axis runs over, the one named last changes fastest.
Arguments:
- observations: float32 [1024, 64], P('tm'), may hold values from -600 to 600
- obs_weights: float32 [1024, 64], P('tm'), may hold values from 0 to 1
- damping: float32 [1024, 256], P('tm'), may hold values from 0.1 to 1
- transition: float32 [256, 256], replicated, may hold values from -1 to 1
- obs_matrix: float32 [64, 256], replicated, may hold values from -0.25 to 0.25
- smoother_gain: float32 [256, 256], replicated, may hold values from -1 to 1
- prior_mean: float32 [256], replicated, may hold values from -6 to 6
Outputs:
- filtered: float32 [1024, 256], P('tm')
- smoothed: float32 [1024, 256], P('tm')
The draws below stay inside these ranges and needn't reach their ends.
All inputs are finite; a program needn't handle non-finite values.
Results may differ from the reference program's by a relative error of at most 0.0003.
Values sent between devices are 32-bit elements; how exact they have to be, the bound alone decides.
No kernel may reach another device: no remote copies, remote signals or barrier semaphores. Data moves between devices by JAX's collectives and lax.ppermute only.
A program may use at most 64 MiB of HBM per device.

```python
import jax
import jax.numpy as jnp
from jax import lax

NS = 256
OBS = 64
STEPS_DEV = 32
STEPS = 1024


highest = lax.Precision.HIGHEST


def rotation_matrix(key, spread):
    raw = jax.random.normal(key, (NS, NS), jnp.float32) / jnp.sqrt(jnp.float32(NS))
    skewed = (raw - raw.T) * (0.5 * spread) / 256.0
    identity = jnp.eye(NS, dtype=jnp.float32)
    term_matrix = identity
    total_matrix = identity
    for order_index in range(1, 11):
        term_matrix = jnp.dot(term_matrix, skewed, precision=highest) / float(order_index)
        total_matrix = total_matrix + term_matrix
    for square_index in range(8):
        total_matrix = jnp.dot(total_matrix, total_matrix, precision=highest)
    return total_matrix


def draw_transition(key, part):
    spread = 0.4
    return rotation_matrix(jax.random.fold_in(key, 101), spread)


def draw_smoother_gain(key, part):
    spread = 0.4
    rate_low = 0.05
    rate_high = 2.0
    base_matrix = rotation_matrix(jax.random.fold_in(key, 101), spread)
    rates = jnp.exp(jax.random.uniform(jax.random.fold_in(key, 202), (NS,), jnp.float32, jnp.log(rate_low), jnp.log(rate_high)))
    keeps = jnp.exp(-rates / float(STEPS))
    return base_matrix.T * keeps[None, :]


def draw_damping(key, part):
    rate_low = 0.05
    rate_high = 2.0
    channel_rates = jnp.exp(jax.random.uniform(jax.random.fold_in(key, 301), (NS,), jnp.float32, jnp.log(rate_low), jnp.log(rate_high)))
    block_rates = jnp.exp(jax.random.uniform(jax.random.fold_in(key, 302), (STEPS // STEPS_DEV, 1), jnp.float32, jnp.log(0.5), jnp.log(2.0)))
    block_rates = jnp.repeat(block_rates, STEPS_DEV, axis=0)
    roughness = jnp.exp(jax.random.uniform(jax.random.fold_in(key, 303), (STEPS, NS), jnp.float32, jnp.log(0.5), jnp.log(2.0)))
    rates = channel_rates[None, :] * block_rates * roughness / float(STEPS)
    positions = jax.random.randint(jax.random.fold_in(key, 304), (3,), 0, STEPS)
    strengths = jax.random.uniform(jax.random.fold_in(key, 305), (3,), jnp.float32, 0.5, 0.8)
    step_ids = lax.broadcasted_iota(jnp.int32, (STEPS, 3), 0)
    factors = jnp.prod(jnp.where(step_ids == positions[None, :], strengths[None, :], 1.0), axis=1)
    return jnp.exp(-rates) * factors[:, None]


def draw_obs_weights(key, part):
    scale_value = float(NS) / float(OBS * STEPS)
    values = jnp.exp(jax.random.uniform(jax.random.fold_in(key, 401), (STEPS, OBS), jnp.float32, jnp.log(0.1), jnp.log(3.0)))
    return values * scale_value


def steps_of(own_key, dims, pieces, low, top_value):
    loudness, own = 1.0, jax.random.fold_in(own_key, 6)
    for axis_at, shards_of in pieces:
        draws = jnp.exp(jax.random.uniform(jax.random.fold_in(own, axis_at), (shards_of,), jnp.float32, low / len(pieces), top_value / len(pieces)))
        loudness = loudness * jnp.repeat(draws, dims[axis_at] // shards_of).reshape([-1 if axis == axis_at else 1 for axis in range(len(dims))])
    return loudness


def gaussian(rng, extent, scale, reach, pieces=(), kind=jnp.bfloat16):
    drawn = jax.random.normal(rng, extent, jnp.float32) * scale
    if len(pieces) > 0:
        drawn = steps_of(rng, extent, pieces, -0.22, 0.18) * drawn
    return jnp.clip(drawn, min=-reach, max=reach).astype(kind)


def setup_inputs(seed: int = 0) -> dict:
    key_list = jax.random.split(jax.random.key(seed), 8)
    return {
        "observations": gaussian(key_list[0], (STEPS, OBS), 100.0, 600.0, ((0, 32),), jnp.float32),
        "obs_weights": draw_obs_weights(jax.random.fold_in(key_list[7], 71), 0),
        "damping": draw_damping(jax.random.fold_in(key_list[7], 71), 0),
        "transition": draw_transition(jax.random.fold_in(key_list[7], 71), 0),
        "obs_matrix": gaussian(key_list[4], (OBS, NS), (2 * NS) ** -0.5, 0.25, (), jnp.float32),
        "smoother_gain": draw_smoother_gain(jax.random.fold_in(key_list[7], 71), 0),
        "prior_mean": gaussian(key_list[6], (NS,), 1.0, 6.0, (), jnp.float32),
    }


highest = lax.Precision.HIGHEST


def product(left, right):
    return jnp.dot(left, right, precision=highest, preferred_element_type=jnp.float32)


def reference(observations, obs_weights, damping, transition, obs_matrix, smoother_gain, prior_mean):
    def update(predicted, obs_row, weight_row):
        innovation = obs_row - product(obs_matrix, predicted)
        return predicted + product(weight_row * innovation, obs_matrix)

    first_mean = update(prior_mean, observations[0], obs_weights[0])

    def forward_step(estimate, inputs):
        obs_row, weight_row, damp_row = inputs
        predicted = product(transition, damp_row * estimate)
        estimate = update(predicted, obs_row, weight_row)
        return estimate, estimate

    _, later_means = lax.scan(forward_step, first_mean, (observations[1:], obs_weights[1:], damping[1:]))
    filtered = jnp.concatenate([first_mean[None, :], later_means], axis=0)

    def backward_step(estimate, mean_row):
        estimate = mean_row + product(smoother_gain, estimate - product(transition, mean_row))
        return estimate, estimate

    _, earlier_smooth = lax.scan(backward_step, filtered[-1], filtered[:-1], reverse=True)
    smoothed = jnp.concatenate([earlier_smooth, filtered[-1:]], axis=0)
    return filtered, smoothed
```

```python
import functools

import jax
import jax.numpy as jnp
from jax import lax
from jax.experimental import pallas as pl
from jax.experimental.pallas import tpu as pltpu
from jax.sharding import PartitionSpec as P

f32, bf16 = jnp.float32, jnp.bfloat16
highest = lax.Precision.HIGHEST
PAD = 8
CHUNKS = 4
PLANE = 8


def exact(left, right):
    return jnp.dot(left, right, precision=highest, preferred_element_type=f32)


def split(value):
    high = value.astype(bf16)
    return high, (value - high.astype(f32)).astype(bf16)


def stack_right(high, low):
    return jnp.concatenate([high, low, high], axis=0)


def dot_split(left, right_stack):
    high, low = split(left)
    return jnp.dot(
        jnp.concatenate([high, high, low], axis=1), right_stack, preferred_element_type=f32
    )


def compose(first, second):
    width = first.shape[1]
    joined = dot_split(first, stack_right(*split(second[:width])))
    return jnp.concatenate([joined[:width], joined[width:] + second[width:]], axis=0)


def eye_map(width):
    rows = lax.broadcasted_iota(jnp.int32, (width + PAD, width), 0)
    cols = lax.broadcasted_iota(jnp.int32, (width + PAD, width), 1)
    return (rows == cols).astype(f32)


def local_kernel(
    obs_ref, weight_ref, damp_ref, trans_ref, obsmat_ref, prior_ref,
    path_ref, chunk_ref, total_ref,
    high_ref, low_ref, state_ref, offset_ref, wide_ref, base_ref,
):
    steps, width = damp_ref.shape
    span = steps // CHUNKS
    is_first = (lax.axis_index("tm") == 0).astype(f32)
    obs_mat = obsmat_ref[...]
    weights = weight_ref[...]
    trans_t = trans_ref[...].T
    base_ref[0] = trans_t
    observed = lax.dot_general(
        trans_t, obs_mat, (((1,), (1,)), ((), ())), precision=highest, preferred_element_type=f32
    )
    base_ref[1] = jnp.concatenate([observed] * 4, axis=1)
    wide_ref[...] = jnp.concatenate([weights] * 4, axis=1)
    obs_high, obs_low = split(obs_mat)
    obs_stack = jnp.concatenate([obs_high, obs_low, obs_high, obs_low], axis=0)
    offsets = exact(weights * obs_ref[...], obs_mat)
    prior = jnp.broadcast_to(prior_ref[...], (PAD, width))
    seen = lax.dot_general(
        prior, obs_mat, (((1,), (1,)), ((), ())), precision=highest, preferred_element_type=f32
    )
    begun = prior - exact(seen * weights[0:1], obs_mat)
    step_ids = lax.broadcasted_iota(jnp.int32, (steps, 1), 0)
    offsets = offsets + jnp.where(step_ids == 0, is_first, 0.0) * begun[0:1]
    offset_ref[...] = offsets

    def make(step, carry):
        scaled = base_ref[1] * wide_ref[pl.ds(step, 1), :]
        high, low = split(scaled)
        half = width // 2
        pieces = jnp.concatenate([high[:, :half], low[:, half:]], axis=1)
        moved = base_ref[0] - jnp.dot(pieces, obs_stack, preferred_element_type=f32)
        high, low = split(moved)
        high_ref[step] = high
        low_ref[step] = low
        return carry

    lax.fori_loop(0, steps, make, 0, unroll=2)

    identity = eye_map(width)
    for chunk in range(CHUNKS):
        state_ref[chunk] = identity * (1.0 - is_first) if chunk == 0 else identity

    def advance(step, carry):
        for chunk in range(CHUNKS):
            time = chunk * span + step
            damped = state_ref[chunk] * damp_ref[pl.ds(time, 1), :]
            moved = dot_split(damped, stack_right(high_ref[time], low_ref[time]))
            moved = jnp.concatenate(
                [moved[:width], moved[width:] + offset_ref[pl.ds(time, 1), :]], axis=0
            )
            state_ref[chunk] = moved
            path_ref[time] = moved
        return carry

    lax.fori_loop(0, span, advance, 0)

    entering = state_ref[0]
    for chunk in range(1, CHUNKS):
        chunk_ref[chunk - 1] = entering
        entering = compose(entering, state_ref[chunk])
    total_ref[...] = entering


def pair_kernel(mine_ref, other_ref, chip_ref, half_ref):
    core = lax.axis_index("tm") % 2
    mine, other = mine_ref[...], other_ref[...]
    upper = core == 1
    whole = compose(jnp.where(upper, other, mine), jnp.where(upper, mine, other))
    chip_ref[...] = whole
    half = whole.shape[1] // 2
    half_ref[...] = jnp.where(upper, whole[:, half:], whole[:, :half])


def plane_kernel(chip_ref, mine_ref, other_ref, plane_ref, before_ref, all_ref, prefix_ref):
    me = lax.axis_index("tm")
    upper = me % 2 == 1
    place = (me // 2) % 4
    half = chip_ref.shape[1] // 2
    all_ref[place] = chip_ref[...]
    for distance in range(1, 4):
        mine, other = mine_ref[distance - 1], other_ref[distance - 1]
        all_ref[place ^ distance, :, :half] = jnp.where(upper, other, mine)
        all_ref[place ^ distance, :, half:] = jnp.where(upper, mine, other)
    running = all_ref[0]
    prefix_ref[0] = eye_map(chip_ref.shape[1])
    for position in range(1, 4):
        prefix_ref[position] = running
        running = compose(running, all_ref[position])
    plane_ref[...] = running
    before_ref[...] = prefix_ref[place]


def entry_kernel(before_ref, other_ref, chunk_ref, entry_ref):
    upper = lax.axis_index("tm") % 2 == 1
    before = before_ref[...]
    joined = compose(before, other_ref[...])
    start = jnp.where(upper, joined, before)
    entry_ref[0] = start
    for chunk in range(1, CHUNKS):
        entry_ref[chunk] = compose(start, chunk_ref[chunk - 1])


def power_kernel(trans_ref, gain_ref, mix_ref, high_ref, low_ref):
    gain_t = gain_ref[...].T
    mix_high, mix_low = split(exact(trans_ref[...].T, gain_t))
    mix_ref[...] = stack_right(mix_high, mix_low)
    power = gain_t
    for level in range(high_ref.shape[0]):
        high_ref[level], low_ref[level] = split(power)
        if level + 1 < high_ref.shape[0]:
            power = exact(power, power)


def suffix_scan(rows, high_ref, low_ref, first_level, levels):
    count, width = rows.shape
    for level in range(levels):
        distance = 1 << level
        later = jnp.concatenate(
            [rows[distance:], jnp.zeros((distance, width), f32)], axis=0
        )
        right = stack_right(high_ref[first_level + level], low_ref[first_level + level])
        rows = rows + dot_split(later, right)
    return rows


def filter_kernel(
    enter_ref, entry_ref, path_ref, mix_ref, high_ref, low_ref,
    filtered_ref, local_ref, *, levels
):
    steps, _, width = path_ref.shape
    span = steps // CHUNKS
    is_final = lax.axis_index("tm") == lax.axis_size("tm") - 1
    column = jnp.broadcast_to(enter_ref[0:1], (PAD, width)).T[:, 0:1]
    for chunk in range(CHUNKS):
        entry = entry_ref[chunk]
        start = jnp.sum(entry[:width] * column, axis=0, keepdims=True) + entry[width : width + 1]
        begin = jnp.broadcast_to(start, (PAD, width)).T[:, 0:1]
        for step in range(chunk * span, (chunk + 1) * span):
            path = path_ref[step, :width]
            filtered_ref[step : step + 1] = (
                jnp.sum(path * begin, axis=0, keepdims=True) + path_ref[step, width : width + 1]
            )
    filtered = filtered_ref[...]
    step_ids = lax.broadcasted_iota(jnp.int32, (steps, 1), 0)
    keep = jnp.where(jnp.logical_and(step_ids == steps - 1, is_final), 0.0, 1.0)
    change = filtered - keep * dot_split(filtered, mix_ref[...])
    local_ref[...] = suffix_scan(change, high_ref, low_ref, 0, levels)


def smooth_kernel(all_ref, local_ref, high_ref, low_ref, out_ref, sum_ref, *, levels):
    count, width = all_ref.shape
    steps = local_ref.shape[0]
    me = lax.axis_index("tm")
    sum_ref[pl.ds(count, PAD), :] = jnp.zeros((PAD, width), f32)
    sum_ref[pl.ds(0, count), :] = suffix_scan(
        all_ref[...], high_ref, low_ref, levels, (count - 1).bit_length()
    )
    incoming = jnp.broadcast_to(sum_ref[pl.ds(me + 1, 1), :], (PAD, width))
    lifted = dot_split(incoming, stack_right(high_ref[0], low_ref[0]))[0:1]
    step_ids = lax.broadcasted_iota(jnp.int32, (steps, 1), 0)
    rows = jnp.where(step_ids == steps - 1, lifted, 0.0)
    out_ref[...] = local_ref[...] + suffix_scan(rows, high_ref, low_ref, 0, levels)


def call(kernel, outs, scratch=(), flops=0, limit=16):
    return pl.pallas_call(
        kernel,
        out_shape=outs,
        scratch_shapes=scratch,
        compiler_params=pltpu.CompilerParams(vmem_limit_bytes=limit << 20),
        cost_estimate=pl.CostEstimate(flops=flops, bytes_accessed=1 << 20, transcendentals=0),
    )


def swap(count, distance):
    return [(index, index ^ distance) for index in range(count)]


def per_device(
    observations, obs_weights, damping, transition, obs_matrix, smoother_gain, prior_mean
):
    steps, width = damping.shape
    count = lax.axis_size("tm")
    rows = width + PAD
    levels = (steps - 1).bit_length()
    cube = 2 * width**3

    def struct(*shape, dtype=f32):
        return jax.ShapeDtypeStruct(shape, dtype)

    path, chunk_maps, total = call(
        local_kernel,
        (struct(steps, rows, width), struct(CHUNKS - 1, rows, width), struct(rows, width)),
        (
            pltpu.VMEM((steps, width, width), bf16),
            pltpu.VMEM((steps, width, width), bf16),
            pltpu.VMEM((CHUNKS, rows, width), f32),
            pltpu.VMEM((steps, width), f32),
            pltpu.VMEM((steps, width), f32),
            pltpu.VMEM((2, width, width), f32),
        ),
        flops=130 * cube,
        limit=36,
    )(observations, obs_weights, damping, transition, obs_matrix, prior_mean[None, :])

    power_count = levels + max((count - 1).bit_length(), 1)
    mix, power_high, power_low = call(
        power_kernel,
        (
            struct(3 * width, width, dtype=bf16),
            struct(power_count, width, width, dtype=bf16),
            struct(power_count, width, width, dtype=bf16),
        ),
        flops=60 * cube,
    )(transition, smoother_gain)

    partner = lax.ppermute(total, "tm", swap(count, 1))
    chip, half = call(
        pair_kernel, (struct(rows, width), struct(rows, width // 2)), flops=3 * cube
    )(total, partner)

    halves = jnp.stack(
        [lax.ppermute(half, "tm", swap(count, 2 * distance)) for distance in range(1, 4)]
    )
    other_halves = lax.ppermute(halves, "tm", swap(count, 1))
    plane, before = call(
        plane_kernel,
        (struct(rows, width), struct(rows, width)),
        (pltpu.VMEM((4, rows, width), f32), pltpu.VMEM((4, rows, width), f32)),
        flops=9 * cube,
    )(chip, halves, other_halves)
    entry = call(entry_kernel, struct(CHUNKS, rows, width), flops=12 * cube)(
        before, partner, chunk_maps
    )

    group = lax.axis_index("tm") // PLANE
    enter = jnp.zeros((1, width), f32)
    for hop in range(count // PLANE - 1):
        leave = jnp.sum(plane[:width] * enter.T, axis=0, keepdims=True) + plane[width : width + 1]
        low, high = hop * PLANE, (hop + 1) * PLANE
        pairs = [(low + i, high + i) for i in range(PLANE)]
        pairs = pairs + [(b, a) for a, b in pairs]
        enter = jnp.where(group == hop + 1, lax.ppermute(leave, "tm", pairs), enter)

    filtered, local = call(
        functools.partial(filter_kernel, levels=levels),
        (struct(steps, width), struct(steps, width)),
        flops=20 * cube,
        limit=32,
    )(enter, entry, path, mix, power_high, power_low)

    sent = jnp.broadcast_to(local[0:1], (count, width))
    offsets = lax.all_to_all(sent, "tm", 0, 0, tiled=True)
    smoothed = call(
        functools.partial(smooth_kernel, levels=levels),
        struct(steps, width),
        (pltpu.VMEM((count + PAD, width), f32),),
        flops=20 * cube,
    )(offsets, local, power_high, power_low)
    return filtered, smoothed


def solution(mesh):
    return jax.shard_map(
        per_device,
        mesh=mesh,
        in_specs=(P("tm", None), P("tm", None), P("tm", None), P(), P(), P(), P()),
        out_specs=(P("tm", None), P("tm", None)),
        check_vma=False,
    )
```

```python
import functools

import jax
import jax.numpy as jnp
from jax import lax
from jax.experimental import pallas as pl
from jax.experimental.pallas import tpu as pltpu
from jax.sharding import PartitionSpec as P

f32, bf16 = jnp.float32, jnp.bfloat16
highest = lax.Precision.HIGHEST
PAD = 8
CHUNKS = 4
PLANE = 8


def exact(left, right):
    return jnp.dot(left, right, precision=highest, preferred_element_type=f32)


def split(value):
    high = value.astype(bf16)
    return high, (value - high.astype(f32)).astype(bf16)


def stack_right(high, low):
    return jnp.concatenate([high, low, high], axis=0)


def dot_split(left, right_stack):
    high, low = split(left)
    return jnp.dot(
        jnp.concatenate([high, high, low], axis=1), right_stack, preferred_element_type=f32
    )


def compose(first, second):
    width = first.shape[1]
    joined = dot_split(first, stack_right(*split(second[:width])))
    return jnp.concatenate([joined[:width], joined[width:] + second[width:]], axis=0)


def eye_map(width):
    rows = lax.broadcasted_iota(jnp.int32, (width + PAD, width), 0)
    cols = lax.broadcasted_iota(jnp.int32, (width + PAD, width), 1)
    return (rows == cols).astype(f32)


def fetch(sources, targets, sems):
    copies = [
        pltpu.make_async_copy(source, target, sems.at[index])
        for index, (source, target) in enumerate(zip(sources, targets))
    ]
    for copy in copies:
        copy.start()
    for copy in copies:
        copy.wait()


def local_kernel(
    obs_hbm, weight_hbm, damp_hbm, trans_hbm, obsmat_hbm, prior_hbm,
    path_ref, chunk_ref, total_ref,
    high_ref, low_ref, state_ref, offset_ref, wide_ref, base_ref,
    obs_ref, weight_ref, damp_ref, trans_ref, obsmat_ref, prior_ref, sems,
):
    fetch(
        (trans_hbm, obsmat_hbm, damp_hbm, weight_hbm, obs_hbm, prior_hbm),
        (trans_ref, obsmat_ref, damp_ref, weight_ref, obs_ref, prior_ref),
        sems,
    )
    steps, width = damp_ref.shape
    span = steps // CHUNKS
    is_first = (lax.axis_index("tm") == 0).astype(f32)
    obs_mat = obsmat_ref[...]
    weights = weight_ref[...]
    trans_t = trans_ref[...].T
    base_ref[0] = trans_t
    observed = lax.dot_general(
        trans_t, obs_mat, (((1,), (1,)), ((), ())), precision=highest, preferred_element_type=f32
    )
    base_ref[1] = jnp.concatenate([observed] * 4, axis=1)
    wide_ref[...] = jnp.concatenate([weights] * 4, axis=1)
    obs_high, obs_low = split(obs_mat)
    obs_stack = jnp.concatenate([obs_high, obs_low, obs_high, obs_low], axis=0)
    offsets = exact(weights * obs_ref[...], obs_mat)
    prior = jnp.broadcast_to(prior_ref[...], (PAD, width))
    seen = lax.dot_general(
        prior, obs_mat, (((1,), (1,)), ((), ())), precision=highest, preferred_element_type=f32
    )
    begun = prior - exact(seen * weights[0:1], obs_mat)
    step_ids = lax.broadcasted_iota(jnp.int32, (steps, 1), 0)
    offsets = offsets + jnp.where(step_ids == 0, is_first, 0.0) * begun[0:1]
    offset_ref[...] = offsets

    def make(step, carry):
        scaled = base_ref[1] * wide_ref[pl.ds(step, 1), :]
        high, low = split(scaled)
        half = width // 2
        pieces = jnp.concatenate([high[:, :half], low[:, half:]], axis=1)
        moved = base_ref[0] - jnp.dot(pieces, obs_stack, preferred_element_type=f32)
        high, low = split(moved)
        high_ref[step] = high
        low_ref[step] = low
        return carry

    lax.fori_loop(0, steps, make, 0, unroll=2)

    identity = eye_map(width)
    for chunk in range(CHUNKS):
        state_ref[chunk] = identity * (1.0 - is_first) if chunk == 0 else identity

    def advance(step, carry):
        for chunk in range(CHUNKS):
            time = chunk * span + step
            damped = state_ref[chunk] * damp_ref[pl.ds(time, 1), :]
            moved = dot_split(damped, stack_right(high_ref[time], low_ref[time]))
            moved = jnp.concatenate(
                [moved[:width], moved[width:] + offset_ref[pl.ds(time, 1), :]], axis=0
            )
            state_ref[chunk] = moved
            path_ref[time] = moved
        return carry

    lax.fori_loop(0, span, advance, 0)

    entering = state_ref[0]
    for chunk in range(1, CHUNKS):
        chunk_ref[chunk - 1] = entering
        entering = compose(entering, state_ref[chunk])
    total_ref[...] = entering


def pair_kernel(mine_ref, other_ref, chip_ref, half_ref):
    core = lax.axis_index("tm") % 2
    mine, other = mine_ref[...], other_ref[...]
    upper = core == 1
    whole = compose(jnp.where(upper, other, mine), jnp.where(upper, mine, other))
    chip_ref[...] = whole
    half = whole.shape[1] // 2
    half_ref[...] = jnp.where(upper, whole[:, half:], whole[:, :half])


def plane_kernel(
    chip_ref, mine_ref, other_ref, _, plane_ref, before_ref, leave_ref, all_ref, prefix_ref
):
    me = lax.axis_index("tm")
    upper = me % 2 == 1
    place = (me // 2) % 4
    half = chip_ref.shape[1] // 2
    all_ref[place] = chip_ref[...]
    for distance in range(1, 4):
        mine, other = mine_ref[distance - 1], other_ref[distance - 1]
        all_ref[place ^ distance, :, :half] = jnp.where(upper, other, mine)
        all_ref[place ^ distance, :, half:] = jnp.where(upper, mine, other)
    running = all_ref[0]
    prefix_ref[0] = eye_map(chip_ref.shape[1])
    for position in range(1, 4):
        prefix_ref[position] = running
        running = compose(running, all_ref[position])
    plane_ref[...] = running
    leave_ref[...] = running[chip_ref.shape[1] :]
    before_ref[...] = prefix_ref[place]


def as_column(rows):
    return rows.T[:, 0:1]


def hop_kernel(plane_ref, came_ref, enter_ref, leave_ref, next_ref, *, hop):
    width = plane_ref.shape[1]
    here = lax.axis_index("tm") // PLANE == hop
    enter = jnp.where(here, came_ref[...], enter_ref[...])
    next_ref[...] = enter
    moved = jnp.sum(plane_ref[:width] * as_column(enter), axis=0, keepdims=True)
    leave_ref[...] = moved + plane_ref[width:]


def entry_kernel(before_ref, other_ref, chunk_ref, entry_ref):
    upper = lax.axis_index("tm") % 2 == 1
    before = before_ref[...]
    joined = compose(before, other_ref[...])
    start = jnp.where(upper, joined, before)
    entry_ref[0] = start
    for chunk in range(1, CHUNKS):
        entry_ref[chunk] = compose(start, chunk_ref[chunk - 1])


def power_kernel(trans_hbm, gain_hbm, _, mix_ref, high_ref, low_ref, trans_ref, gain_ref, sems):
    fetch((trans_hbm, gain_hbm), (trans_ref, gain_ref), sems)
    gain_t = gain_ref[...].T
    mix_high, mix_low = split(exact(trans_ref[...].T, gain_t))
    mix_ref[...] = stack_right(mix_high, mix_low)
    power = gain_t
    for level in range(high_ref.shape[0]):
        high_ref[level], low_ref[level] = split(power)
        if level + 1 < high_ref.shape[0]:
            power = exact(power, power)


def suffix_scan(rows, high_ref, low_ref, first_level, levels):
    count, width = rows.shape
    for level in range(levels):
        distance = 1 << level
        later = jnp.concatenate(
            [rows[distance:], jnp.zeros((distance, width), f32)], axis=0
        )
        right = stack_right(high_ref[first_level + level], low_ref[first_level + level])
        rows = rows + dot_split(later, right)
    return rows


def filter_kernel(
    came_ref, enter_ref, entry_ref, path_ref, mix_ref, high_ref, low_ref,
    filtered_ref, local_ref, *, levels, hop
):
    steps, _, width = path_ref.shape
    span = steps // CHUNKS
    is_final = lax.axis_index("tm") == lax.axis_size("tm") - 1
    here = lax.axis_index("tm") // PLANE == hop
    column = as_column(jnp.where(here, came_ref[...], enter_ref[...]))
    for chunk in range(CHUNKS):
        entry = entry_ref[chunk]
        start = jnp.sum(entry[:width] * column, axis=0, keepdims=True) + entry[width : width + 1]
        begin = as_column(jnp.broadcast_to(start, (PAD, width)))
        for step in range(chunk * span, (chunk + 1) * span):
            path = path_ref[step, :width]
            filtered_ref[step : step + 1] = (
                jnp.sum(path * begin, axis=0, keepdims=True) + path_ref[step, width : width + 1]
            )
    filtered = filtered_ref[...]
    step_ids = lax.broadcasted_iota(jnp.int32, (steps, 1), 0)
    keep = jnp.where(jnp.logical_and(step_ids == steps - 1, is_final), 0.0, 1.0)
    change = filtered - keep * dot_split(filtered, mix_ref[...])
    local_ref[...] = suffix_scan(change, high_ref, low_ref, 0, levels)


def smooth_kernel(all_ref, local_ref, high_ref, low_ref, out_ref, sum_ref, *, levels):
    count, width = all_ref.shape
    steps = local_ref.shape[0]
    me = lax.axis_index("tm")
    sum_ref[pl.ds(count, PAD), :] = jnp.zeros((PAD, width), f32)
    sum_ref[pl.ds(0, count), :] = suffix_scan(
        all_ref[...], high_ref, low_ref, levels, (count - 1).bit_length()
    )
    incoming = jnp.broadcast_to(sum_ref[pl.ds(me + 1, 1), :], (PAD, width))
    lifted = dot_split(incoming, stack_right(high_ref[0], low_ref[0]))[0:1]
    step_ids = lax.broadcasted_iota(jnp.int32, (steps, 1), 0)
    rows = jnp.where(step_ids == steps - 1, lifted, 0.0)
    out_ref[...] = local_ref[...] + suffix_scan(rows, high_ref, low_ref, 0, levels)


def call(kernel, outs, scratch=(), flops=0, limit=8, spaces=None):
    extra = {} if spaces is None else {"in_specs": [pl.BlockSpec(memory_space=s) for s in spaces]}
    return pl.pallas_call(
        kernel,
        out_shape=outs,
        **extra,
        scratch_shapes=scratch,
        compiler_params=pltpu.CompilerParams(vmem_limit_bytes=limit << 20),
        cost_estimate=pl.CostEstimate(flops=flops, bytes_accessed=1 << 20, transcendentals=0),
    )


def swap(count, distance):
    return [(index, index ^ distance) for index in range(count)]


def per_device(
    observations, obs_weights, damping, transition, obs_matrix, smoother_gain, prior_mean
):
    steps, width = damping.shape
    count = lax.axis_size("tm")
    rows = width + PAD
    levels = (steps - 1).bit_length()
    cube = 2 * width**3

    def struct(*shape, dtype=f32):
        return jax.ShapeDtypeStruct(shape, dtype)

    path, chunk_maps, total = call(
        local_kernel,
        (struct(steps, rows, width), struct(CHUNKS - 1, rows, width), struct(rows, width)),
        (
            pltpu.VMEM((steps, width, width), bf16),
            pltpu.VMEM((steps, width, width), bf16),
            pltpu.VMEM((CHUNKS, rows, width), f32),
            pltpu.VMEM((steps, width), f32),
            pltpu.VMEM((steps, width), f32),
            pltpu.VMEM((2, width, width), f32),
            pltpu.VMEM(observations.shape, f32),
            pltpu.VMEM(obs_weights.shape, f32),
            pltpu.VMEM(damping.shape, f32),
            pltpu.VMEM(transition.shape, f32),
            pltpu.VMEM(obs_matrix.shape, f32),
            pltpu.VMEM((1, width), f32),
            pltpu.SemaphoreType.DMA((6,)),
        ),
        flops=130 * cube,
        limit=32,
        spaces=[pltpu.HBM] * 6,
    )(observations, obs_weights, damping, transition, obs_matrix, prior_mean[None, :])

    partner = lax.ppermute(total, "tm", swap(count, 1))
    chip, half = call(
        pair_kernel, (struct(rows, width), struct(rows, width // 2)), flops=3 * cube
    )(total, partner)

    halves = jnp.stack(
        [lax.ppermute(half, "tm", swap(count, 2 * distance)) for distance in range(1, 4)]
    )
    other_halves = lax.ppermute(halves, "tm", swap(count, 1))
    power_count = levels + max((count - 1).bit_length(), 1)
    mix, power_high, power_low = call(
        power_kernel,
        (
            struct(3 * width, width, dtype=bf16),
            struct(power_count, width, width, dtype=bf16),
            struct(power_count, width, width, dtype=bf16),
        ),
        (
            pltpu.VMEM(transition.shape, f32),
            pltpu.VMEM(transition.shape, f32),
            pltpu.SemaphoreType.DMA((2,)),
        ),
        flops=60 * cube,
        spaces=[pltpu.HBM, pltpu.HBM, pl.ANY],
    )(transition, smoother_gain, half)
    plane, before, leave = call(
        plane_kernel,
        (struct(rows, width), struct(rows, width), struct(PAD, width)),
        (pltpu.VMEM((4, rows, width), f32), pltpu.VMEM((4, rows, width), f32)),
        flops=9 * cube,
        spaces=[pltpu.VMEM] * 3 + [pl.ANY],
    )(chip, halves, other_halves, mix)
    entry = call(entry_kernel, struct(CHUNKS, rows, width), flops=12 * cube)(
        before, partner, chunk_maps
    )

    enter = jnp.zeros((PAD, width), f32)
    came = leave
    hops = count // PLANE - 1
    for hop in range(hops):
        if hop > 0:
            leave, enter = call(
                functools.partial(hop_kernel, hop=hop),
                (struct(PAD, width), struct(PAD, width)),
                flops=cube // 64,
                limit=2,
            )(plane, came, enter)
        low, high = hop * PLANE, (hop + 1) * PLANE
        pairs = [(low + i, high + i) for i in range(PLANE)]
        pairs = pairs + [(b, a) for a, b in pairs]
        came = lax.ppermute(leave, "tm", pairs)

    filtered, local = call(
        functools.partial(filter_kernel, levels=levels, hop=hops),
        (struct(steps, width), struct(steps, width)),
        flops=20 * cube,
    )(came, enter, entry, path, mix, power_high, power_low)

    sent = jnp.broadcast_to(local[0:1], (count, width))
    offsets = lax.all_to_all(sent, "tm", 0, 0, tiled=True)
    smoothed = call(
        functools.partial(smooth_kernel, levels=levels),
        struct(steps, width),
        (pltpu.VMEM((count + PAD, width), f32),),
        flops=20 * cube,
    )(offsets, local, power_high, power_low)
    return filtered, smoothed


def solution(mesh):
    return jax.shard_map(
        per_device,
        mesh=mesh,
        in_specs=(P("tm", None), P("tm", None), P("tm", None), P(), P(), P(), P()),
        out_specs=(P("tm", None), P("tm", None)),
        check_vma=False,
    )
```

```python
import functools

import jax
import jax.numpy as jnp
from jax import lax
from jax.experimental import pallas as pl
from jax.experimental.pallas import tpu as pltpu
from jax.sharding import PartitionSpec as P

f32, bf16 = jnp.float32, jnp.bfloat16
highest = lax.Precision.HIGHEST
PAD = 8
CHUNKS = 4
PLANE = 8


def exact(left, right):
    return jnp.dot(left, right, precision=highest, preferred_element_type=f32)


def split(value):
    high = value.astype(bf16)
    return high, (value - high.astype(f32)).astype(bf16)


def stack_right(high, low):
    return jnp.concatenate([high, low, high], axis=0)


def dot_split(left, right_stack):
    high, low = split(left)
    return jnp.dot(
        jnp.concatenate([high, high, low], axis=1), right_stack, preferred_element_type=f32
    )


def compose(first, second):
    width = first.shape[1]
    joined = dot_split(first, stack_right(*split(second[:width])))
    return jnp.concatenate([joined[:width], joined[width:] + second[width:]], axis=0)


def eye_map(width):
    rows = lax.broadcasted_iota(jnp.int32, (width + PAD, width), 0)
    cols = lax.broadcasted_iota(jnp.int32, (width + PAD, width), 1)
    return (rows == cols).astype(f32)


def as_column(rows):
    return rows.T[:, 0:1]


def fetch(sources, targets, sems):
    copies = [
        pltpu.make_async_copy(source, target, sems.at[index])
        for index, (source, target) in enumerate(zip(sources, targets))
    ]
    for copy in copies:
        copy.start()
    for copy in copies:
        copy.wait()


def local_kernel(
    obs_hbm, weight_hbm, damp_hbm, trans_hbm, obsmat_hbm, prior_hbm,
    path_ref, chunk_ref, total_ref,
    high_even, low_even, high_odd, low_odd, state_ref, offset_ref, wide_ref, base_ref,
    obs_ref, weight_ref, damp_ref, trans_ref, obsmat_ref, prior_ref, sems,
):
    fetch(
        (trans_hbm, obsmat_hbm, damp_hbm, weight_hbm, obs_hbm, prior_hbm),
        (trans_ref, obsmat_ref, damp_ref, weight_ref, obs_ref, prior_ref),
        sems,
    )
    steps, width = damp_ref.shape
    span = steps // CHUNKS
    is_first = (lax.axis_index("tm") == 0).astype(f32)
    obs_mat = obsmat_ref[...]
    weights = weight_ref[...]
    trans_t = trans_ref[...].T
    base_ref[0] = trans_t
    observed = lax.dot_general(
        trans_t, obs_mat, (((1,), (1,)), ((), ())), precision=highest, preferred_element_type=f32
    )
    base_ref[1] = jnp.concatenate([observed] * 4, axis=1)
    wide_ref[...] = jnp.concatenate([weights] * 4, axis=1)
    obs_high, obs_low = split(obs_mat)
    obs_stack = jnp.concatenate([obs_high, obs_low, obs_high, obs_low], axis=0)
    offsets = exact(weights * obs_ref[...], obs_mat)
    prior = jnp.broadcast_to(prior_ref[...], (PAD, width))
    seen = lax.dot_general(
        prior, obs_mat, (((1,), (1,)), ((), ())), precision=highest, preferred_element_type=f32
    )
    begun = prior - exact(seen * weights[0:1], obs_mat)
    step_ids = lax.broadcasted_iota(jnp.int32, (steps, 1), 0)
    offsets = offsets + jnp.where(step_ids == 0, is_first, 0.0) * begun[0:1]
    offset_ref[...] = offsets

    half = width // 2

    def make(time):
        scaled = base_ref[1] * wide_ref[pl.ds(time, 1), :]
        high, low = split(scaled)
        pieces = jnp.concatenate([high[:, :half], low[:, half:]], axis=1)
        return base_ref[0] - jnp.dot(pieces, obs_stack, preferred_element_type=f32)

    for chunk in range(CHUNKS):
        time = chunk * span
        damp = as_column(jnp.broadcast_to(damp_ref[time : time + 1], (PAD, width)))
        begin = make(time) * damp
        if chunk == 0:
            begin = begin * (1.0 - is_first)
        moved = jnp.concatenate(
            [begin, jnp.broadcast_to(offset_ref[time : time + 1], (PAD, width))], axis=0
        )
        state_ref[chunk] = moved
        path_ref[time] = moved

    def ready(step, chunk, slot):
        slot[0][chunk], slot[1][chunk] = split(make(chunk * span + step))

    def advance(step, slot, following):
        for chunk in range(CHUNKS):
            time = chunk * span + step
            damped = state_ref[chunk] * damp_ref[pl.ds(time, 1), :]
            moved = dot_split(damped, stack_right(slot[0][chunk], slot[1][chunk]))
            moved = jnp.concatenate(
                [moved[:width], moved[width:] + offset_ref[pl.ds(time, 1), :]], axis=0
            )
            state_ref[chunk] = moved
            path_ref[time] = moved
            if following is not None:
                ready(step + 1, chunk, following)

    even, odd = (high_even, low_even), (high_odd, low_odd)
    for chunk in range(CHUNKS):
        ready(1, chunk, odd)

    def two(index, carry):
        advance(2 * index + 1, odd, even)
        advance(2 * index + 2, even, odd)
        return carry

    lax.fori_loop(0, span // 2 - 1, two, 0)
    advance(span - 1, odd, None)

    first = compose(state_ref[0], state_ref[1])
    chunk_ref[0] = state_ref[0]
    chunk_ref[1] = first
    chunk_ref[2] = state_ref[2]
    total_ref[...] = compose(first, compose(state_ref[2], state_ref[3]))


def pair_kernel(mine_ref, other_ref, chip_ref, half_ref):
    core = lax.axis_index("tm") % 2
    mine, other = mine_ref[...], other_ref[...]
    upper = core == 1
    whole = compose(jnp.where(upper, other, mine), jnp.where(upper, mine, other))
    chip_ref[...] = whole
    half = whole.shape[1] // 2
    half_ref[...] = jnp.where(upper, whole[:, half:], whole[:, :half])


def plane_kernel(
    chip_ref, mine_ref, other_ref, _, plane_ref, before_ref, leave_ref, all_ref, prefix_ref
):
    me = lax.axis_index("tm")
    upper = me % 2 == 1
    place = (me // 2) % 4
    half = chip_ref.shape[1] // 2
    all_ref[place] = chip_ref[...]
    for part in range(2):
        mine, other = mine_ref[part], other_ref[part]
        columns = pl.ds(part * half, half)
        all_ref[place ^ 1, :, columns] = jnp.where(upper, other, mine)
        all_ref[place ^ 2, :, columns] = jnp.where(upper, mine, other)
    mine, other = mine_ref[2], other_ref[2]
    all_ref[place ^ 3, :, :half] = jnp.where(upper, other, mine)
    all_ref[place ^ 3, :, half:] = jnp.where(upper, mine, other)
    running = all_ref[0]
    prefix_ref[0] = eye_map(chip_ref.shape[1])
    for position in range(1, 4):
        prefix_ref[position] = running
        running = compose(running, all_ref[position])
    plane_ref[...] = running
    leave_ref[...] = running[chip_ref.shape[1] :]
    before_ref[...] = prefix_ref[place]


def hop_kernel(plane_ref, came_ref, enter_ref, leave_ref, next_ref, *, hop):
    width = plane_ref.shape[1]
    here = lax.axis_index("tm") // PLANE == hop
    enter = jnp.where(here, came_ref[...], enter_ref[...])
    next_ref[...] = enter
    moved = jnp.sum(plane_ref[:width] * as_column(enter), axis=0, keepdims=True)
    leave_ref[...] = moved + plane_ref[width:]


def entry_kernel(before_ref, other_ref, chunk_ref, entry_ref):
    upper = lax.axis_index("tm") % 2 == 1
    before = before_ref[...]
    joined = compose(before, other_ref[...])
    start = jnp.where(upper, joined, before)
    entry_ref[0] = start
    entry_ref[1] = compose(start, chunk_ref[0])
    entry_ref[2] = compose(start, chunk_ref[1])
    entry_ref[3] = compose(entry_ref[2], chunk_ref[2])


def power_kernel(trans_hbm, gain_hbm, _, mix_ref, high_ref, low_ref, trans_ref, gain_ref, sems):
    fetch((trans_hbm, gain_hbm), (trans_ref, gain_ref), sems)
    gain_t = gain_ref[...].T
    mix_high, mix_low = split(exact(trans_ref[...].T, gain_t))
    mix_ref[...] = stack_right(mix_high, mix_low)
    power = gain_t
    for level in range(high_ref.shape[0]):
        high_ref[level], low_ref[level] = split(power)
        if level + 1 < high_ref.shape[0]:
            power = exact(power, power)


def suffix_scan(rows, high_ref, low_ref, first_level, levels):
    count, width = rows.shape
    for level in range(levels):
        distance = 1 << level
        later = jnp.concatenate(
            [rows[distance:], jnp.zeros((distance, width), f32)], axis=0
        )
        right = stack_right(high_ref[first_level + level], low_ref[first_level + level])
        rows = rows + dot_split(later, right)
    return rows


def filter_kernel(
    came_ref, enter_ref, entry_ref, path_ref, mix_ref, high_ref, low_ref,
    filtered_ref, local_ref, *, levels, hop
):
    steps, _, width = path_ref.shape
    span = steps // CHUNKS
    is_final = lax.axis_index("tm") == lax.axis_size("tm") - 1
    here = lax.axis_index("tm") // PLANE == hop
    column = as_column(jnp.where(here, came_ref[...], enter_ref[...]))
    for chunk in range(CHUNKS):
        entry = entry_ref[chunk]
        start = jnp.sum(entry[:width] * column, axis=0, keepdims=True) + entry[width : width + 1]
        begin = as_column(jnp.broadcast_to(start, (PAD, width)))
        for step in range(chunk * span, (chunk + 1) * span):
            path = path_ref[step, :width]
            filtered_ref[step : step + 1] = (
                jnp.sum(path * begin, axis=0, keepdims=True) + path_ref[step, width : width + 1]
            )
    filtered = filtered_ref[...]
    step_ids = lax.broadcasted_iota(jnp.int32, (steps, 1), 0)
    keep = jnp.where(jnp.logical_and(step_ids == steps - 1, is_final), 0.0, 1.0)
    change = filtered - keep * dot_split(filtered, mix_ref[...])
    local_ref[...] = suffix_scan(change, high_ref, low_ref, 0, levels)


def smooth_kernel(all_ref, local_ref, high_ref, low_ref, out_ref, sum_ref, *, levels):
    count, width = all_ref.shape
    steps = local_ref.shape[0]
    me = lax.axis_index("tm")
    sum_ref[pl.ds(count, PAD), :] = jnp.zeros((PAD, width), f32)
    sum_ref[pl.ds(0, count), :] = suffix_scan(
        all_ref[...], high_ref, low_ref, levels, (count - 1).bit_length()
    )
    incoming = jnp.broadcast_to(sum_ref[pl.ds(me + 1, 1), :], (PAD, width))
    lifted = dot_split(incoming, stack_right(high_ref[0], low_ref[0]))[0:1]
    step_ids = lax.broadcasted_iota(jnp.int32, (steps, 1), 0)
    rows = jnp.where(step_ids == steps - 1, lifted, 0.0)
    out_ref[...] = local_ref[...] + suffix_scan(rows, high_ref, low_ref, 0, levels)


def call(kernel, outs, scratch=(), flops=0, limit=8, spaces=None):
    extra = {} if spaces is None else {"in_specs": [pl.BlockSpec(memory_space=s) for s in spaces]}
    return pl.pallas_call(
        kernel,
        out_shape=outs,
        **extra,
        scratch_shapes=scratch,
        compiler_params=pltpu.CompilerParams(vmem_limit_bytes=limit << 20),
        cost_estimate=pl.CostEstimate(flops=flops, bytes_accessed=1 << 20, transcendentals=0),
    )


def swap(count, distance):
    return [(index, index ^ distance) for index in range(count)]


def per_device(
    observations, obs_weights, damping, transition, obs_matrix, smoother_gain, prior_mean
):
    observations, obs_weights, damping, transition, obs_matrix, smoother_gain, prior_row = (
        pltpu.with_memory_space_constraint(value, pltpu.HBM)
        for value in (
            observations, obs_weights, damping, transition, obs_matrix, smoother_gain,
            prior_mean[None, :],
        )
    )
    steps, width = damping.shape
    count = lax.axis_size("tm")
    rows = width + PAD
    levels = (steps - 1).bit_length()
    cube = 2 * width**3

    def struct(*shape, dtype=f32):
        return jax.ShapeDtypeStruct(shape, dtype)

    path, chunk_maps, total = call(
        local_kernel,
        (struct(steps, rows, width), struct(CHUNKS - 1, rows, width), struct(rows, width)),
        (
            pltpu.VMEM((CHUNKS, width, width), bf16),
            pltpu.VMEM((CHUNKS, width, width), bf16),
            pltpu.VMEM((CHUNKS, width, width), bf16),
            pltpu.VMEM((CHUNKS, width, width), bf16),
            pltpu.VMEM((CHUNKS, rows, width), f32),
            pltpu.VMEM((steps, width), f32),
            pltpu.VMEM((steps, width), f32),
            pltpu.VMEM((2, width, width), f32),
            pltpu.VMEM(observations.shape, f32),
            pltpu.VMEM(obs_weights.shape, f32),
            pltpu.VMEM(damping.shape, f32),
            pltpu.VMEM(transition.shape, f32),
            pltpu.VMEM(obs_matrix.shape, f32),
            pltpu.VMEM((1, width), f32),
            pltpu.SemaphoreType.DMA((6,)),
        ),
        flops=130 * cube,
        limit=32,
        spaces=[pltpu.HBM] * 6,
    )(observations, obs_weights, damping, transition, obs_matrix, prior_row)

    partner = lax.ppermute(total, "tm", swap(count, 1))
    chip, half = call(
        pair_kernel, (struct(rows, width), struct(rows, width // 2)), flops=3 * cube
    )(total, partner)

    straight = [(index, index ^ (4 if index % 2 else 2)) for index in range(count)]
    diagonal = lax.ppermute(half, "tm", swap(count, 6))
    whole = lax.ppermute(chip, "tm", straight)
    middle = width // 2
    power_count = levels + max((count - 1).bit_length(), 1)
    mix, power_high, power_low = call(
        power_kernel,
        (
            struct(3 * width, width, dtype=bf16),
            struct(power_count, width, width, dtype=bf16),
            struct(power_count, width, width, dtype=bf16),
        ),
        (
            pltpu.VMEM(transition.shape, f32),
            pltpu.VMEM(transition.shape, f32),
            pltpu.SemaphoreType.DMA((2,)),
        ),
        flops=60 * cube,
        spaces=[pltpu.HBM, pltpu.HBM, pl.ANY],
    )(transition, smoother_gain, half)
    whole, diagonal, mix = lax.optimization_barrier((whole, diagonal, mix))
    halves = jnp.stack([whole[:, :middle], whole[:, middle:], diagonal])
    other_halves = lax.ppermute(halves, "tm", swap(count, 1))
    plane, before, leave = call(
        plane_kernel,
        (struct(rows, width), struct(rows, width), struct(PAD, width)),
        (pltpu.VMEM((4, rows, width), f32), pltpu.VMEM((4, rows, width), f32)),
        flops=9 * cube,
        spaces=[pltpu.VMEM] * 3 + [pl.ANY],
    )(chip, halves, other_halves, mix)
    entry = call(entry_kernel, struct(CHUNKS, rows, width), flops=12 * cube)(
        before, partner, chunk_maps
    )

    enter = jnp.zeros((PAD, width), f32)
    came = leave
    hops = count // PLANE - 1
    for hop in range(hops):
        if hop > 0:
            leave, enter = call(
                functools.partial(hop_kernel, hop=hop),
                (struct(PAD, width), struct(PAD, width)),
                flops=cube // 64,
                limit=2,
            )(plane, came, enter)
        low, high = hop * PLANE, (hop + 1) * PLANE
        pairs = [(low + i, high + i) for i in range(PLANE)]
        pairs = pairs + [(b, a) for a, b in pairs]
        came = lax.ppermute(leave, "tm", pairs)

    filtered, local = call(
        functools.partial(filter_kernel, levels=levels, hop=hops),
        (struct(steps, width), struct(steps, width)),
        flops=20 * cube,
    )(came, enter, entry, path, mix, power_high, power_low)

    sent = jnp.broadcast_to(local[0:1], (count, width))
    offsets = lax.all_to_all(sent, "tm", 0, 0, tiled=True)
    smoothed = call(
        functools.partial(smooth_kernel, levels=levels),
        struct(steps, width),
        (pltpu.VMEM((count + PAD, width), f32),),
        flops=20 * cube,
    )(offsets, local, power_high, power_low)
    return filtered, smoothed


def solution(mesh):
    return jax.shard_map(
        per_device,
        mesh=mesh,
        in_specs=(P("tm", None), P("tm", None), P("tm", None), P(), P(), P(), P()),
        out_specs=(P("tm", None), P("tm", None)),
        check_vma=False,
    )
```

```python
import functools

import jax
import jax.numpy as jnp
from jax import lax
from jax.experimental import pallas as pl
from jax.experimental.pallas import tpu as pltpu
from jax.sharding import PartitionSpec as P

f32, bf16 = jnp.float32, jnp.bfloat16
highest = lax.Precision.HIGHEST
PAD = 8
CHUNKS = 4
PLANE = 8


def exact(left, right):
    return jnp.dot(left, right, precision=highest, preferred_element_type=f32)


def split(value):
    high = value.astype(bf16)
    return high, (value - high.astype(f32)).astype(bf16)


def stack_right(high, low):
    return jnp.concatenate([high, low, high], axis=0)


def dot_split(left, right_stack):
    high, low = split(left)
    return jnp.dot(
        jnp.concatenate([high, high, low], axis=1), right_stack, preferred_element_type=f32
    )


def dot_few(left, right_high, right_low):
    count = left.shape[0]
    high, low = split(left)
    stacked = jnp.concatenate(
        [
            jnp.concatenate([high, high], axis=1),
            jnp.concatenate([low, jnp.zeros_like(low)], axis=1),
        ],
        axis=0,
    )
    right = jnp.concatenate([right_high, right_low], axis=0)
    both = jnp.dot(stacked, right, preferred_element_type=f32)
    return both[:count] + both[count:]


def compose(first, second):
    width = first.shape[1]
    joined = dot_split(first, stack_right(*split(second[:width])))
    return jnp.concatenate([joined[:width], joined[width:] + second[width:]], axis=0)


def eye_map(width):
    rows = lax.broadcasted_iota(jnp.int32, (width + PAD, width), 0)
    cols = lax.broadcasted_iota(jnp.int32, (width + PAD, width), 1)
    return (rows == cols).astype(f32)


def as_column(rows):
    return rows.T[:, 0:1]


def fetch(sources, targets, sems):
    copies = [
        pltpu.make_async_copy(source, target, sems.at[index])
        for index, (source, target) in enumerate(zip(sources, targets))
    ]
    for copy in copies:
        copy.start()
    for copy in copies:
        copy.wait()


def local_kernel(
    obs_hbm, weight_hbm, damp_hbm, trans_hbm, obsmat_hbm, prior_hbm,
    path_ref, chunk_ref, total_ref,
    high_even, low_even, high_odd, low_odd, state_ref, offset_ref, wide_ref, base_ref,
    obs_ref, weight_ref, damp_ref, trans_ref, obsmat_ref, prior_ref, sems,
):
    fetch(
        (trans_hbm, obsmat_hbm, damp_hbm, weight_hbm, obs_hbm, prior_hbm),
        (trans_ref, obsmat_ref, damp_ref, weight_ref, obs_ref, prior_ref),
        sems,
    )
    steps, width = damp_ref.shape
    span = steps // CHUNKS
    is_first = (lax.axis_index("tm") == 0).astype(f32)
    obs_mat = obsmat_ref[...]
    weights = weight_ref[...]
    trans_t = trans_ref[...].T
    base_ref[0] = trans_t
    observed = lax.dot_general(
        trans_t, obs_mat, (((1,), (1,)), ((), ())), precision=highest, preferred_element_type=f32
    )
    base_ref[1] = jnp.concatenate([observed] * 4, axis=1)
    wide_ref[...] = jnp.concatenate([weights] * 4, axis=1)
    obs_high, obs_low = split(obs_mat)
    obs_stack = jnp.concatenate([obs_high, obs_low, obs_high, obs_low], axis=0)

    half = width // 2

    def make(time):
        scaled = base_ref[1] * wide_ref[pl.ds(time, 1), :]
        high, low = split(scaled)
        pieces = jnp.concatenate([high[:, :half], low[:, half:]], axis=1)
        return base_ref[0] - jnp.dot(pieces, obs_stack, preferred_element_type=f32)

    for chunk in range(CHUNKS):
        time = chunk * span
        damp = as_column(jnp.broadcast_to(damp_ref[time : time + 1], (PAD, width)))
        begin = make(time) * damp
        if chunk == 0:
            begin = begin * (1.0 - is_first)
        state_ref[chunk, :width] = begin
        path_ref[time, :width] = begin

    def ready(step, chunk, slot):
        slot[0][chunk], slot[1][chunk] = split(make(chunk * span + step))

    def advance(step, slot, following):
        for chunk in range(CHUNKS):
            time = chunk * span + step
            damped = state_ref[chunk] * damp_ref[pl.ds(time, 1), :]
            moved = dot_split(damped, stack_right(slot[0][chunk], slot[1][chunk]))
            moved = jnp.concatenate(
                [moved[:width], moved[width:] + offset_ref[pl.ds(time, 1), :]], axis=0
            )
            state_ref[chunk] = moved
            path_ref[time] = moved
            if following is not None:
                ready(step + 1, chunk, following)

    even, odd = (high_even, low_even), (high_odd, low_odd)
    for chunk in range(CHUNKS):
        ready(1, chunk, odd)

    offsets = exact(weights * obs_ref[...], obs_mat)
    prior = jnp.broadcast_to(prior_ref[...], (PAD, width))
    seen = lax.dot_general(
        prior, obs_mat, (((1,), (1,)), ((), ())), precision=highest, preferred_element_type=f32
    )
    begun = prior - exact(seen * weights[0:1], obs_mat)
    step_ids = lax.broadcasted_iota(jnp.int32, (steps, 1), 0)
    offsets = offsets + jnp.where(step_ids == 0, is_first, 0.0) * begun[0:1]
    offset_ref[...] = offsets
    for chunk in range(CHUNKS):
        time = chunk * span
        begin = jnp.broadcast_to(offsets[time : time + 1], (PAD, width))
        state_ref[chunk, width:] = begin
        path_ref[time, width:] = begin

    def two(index, carry):
        advance(2 * index + 1, odd, even)
        advance(2 * index + 2, even, odd)
        return carry

    lax.fori_loop(0, span // 2 - 1, two, 0)
    advance(span - 1, odd, None)

    first = compose(state_ref[0], state_ref[1])
    chunk_ref[0] = state_ref[0]
    chunk_ref[1] = first
    chunk_ref[2] = state_ref[2]
    total_ref[...] = compose(first, compose(state_ref[2], state_ref[3]))


def pair_kernel(mine_ref, other_ref, chip_ref, half_ref):
    core = lax.axis_index("tm") % 2
    mine, other = mine_ref[...], other_ref[...]
    upper = core == 1
    whole = compose(jnp.where(upper, other, mine), jnp.where(upper, mine, other))
    chip_ref[...] = whole
    half = whole.shape[1] // 2
    half_ref[...] = jnp.where(upper, whole[:, half:], whole[:, :half])


def plane_kernel(
    chip_ref, mine_ref, other_ref, _, plane_ref, before_ref, leave_ref, all_ref, prefix_ref
):
    me = lax.axis_index("tm")
    upper = me % 2 == 1
    place = (me // 2) % 4
    half = chip_ref.shape[1] // 2
    all_ref[place] = chip_ref[...]
    for part in range(2):
        mine, other = mine_ref[part], other_ref[part]
        columns = pl.ds(part * half, half)
        all_ref[place ^ 1, :, columns] = jnp.where(upper, other, mine)
        all_ref[place ^ 2, :, columns] = jnp.where(upper, mine, other)
    mine, other = mine_ref[2], other_ref[2]
    all_ref[place ^ 3, :, :half] = jnp.where(upper, other, mine)
    all_ref[place ^ 3, :, half:] = jnp.where(upper, mine, other)
    width = chip_ref.shape[1]
    left = compose(all_ref[0], all_ref[1])
    right = compose(all_ref[2], all_ref[3])
    whole = compose(left, right)
    plane_ref[...] = whole
    leave_ref[...] = whole[width:]
    prefix_ref[0] = eye_map(width)
    prefix_ref[1] = all_ref[0]
    prefix_ref[2] = left
    prefix_ref[3] = compose(left, all_ref[2])
    before_ref[...] = prefix_ref[place]


def hop_kernel(plane_ref, came_ref, enter_ref, leave_ref, next_ref, *, hop):
    width = plane_ref.shape[1]
    here = lax.axis_index("tm") // PLANE == hop
    enter = jnp.where(here, came_ref[...], enter_ref[...])
    next_ref[...] = enter
    moved = jnp.sum(plane_ref[:width] * as_column(enter), axis=0, keepdims=True)
    leave_ref[...] = moved + plane_ref[width:]


def entry_kernel(before_ref, other_ref, chunk_ref, entry_ref):
    upper = lax.axis_index("tm") % 2 == 1
    before = before_ref[...]
    joined = compose(before, other_ref[...])
    start = jnp.where(upper, joined, before)
    entry_ref[0] = start
    entry_ref[1] = compose(start, chunk_ref[0])
    entry_ref[2] = compose(start, chunk_ref[1])
    entry_ref[3] = compose(entry_ref[2], chunk_ref[2])


def power_kernel(trans_hbm, gain_hbm, _, mix_ref, high_ref, low_ref, trans_ref, gain_ref, sems):
    fetch((trans_hbm, gain_hbm), (trans_ref, gain_ref), sems)
    gain_t = gain_ref[...].T
    mix_high, mix_low = split(exact(trans_ref[...].T, gain_t))
    mix_ref[...] = stack_right(mix_high, mix_low)
    power = gain_t
    for level in range(high_ref.shape[0]):
        high_ref[level], low_ref[level] = split(power)
        if level + 1 < high_ref.shape[0]:
            power = exact(power, power)


def suffix_scan(rows, high_ref, low_ref, first_level, levels):
    count, width = rows.shape
    for level in range(levels):
        distance = 1 << level
        later = jnp.concatenate(
            [rows[distance:], jnp.zeros((distance, width), f32)], axis=0
        )
        rows = rows + dot_few(later, high_ref[first_level + level], low_ref[first_level + level])
    return rows


def filter_kernel(
    came_ref, enter_ref, entry_ref, path_ref, mix_ref, high_ref, low_ref,
    filtered_ref, local_ref, *, levels, hop
):
    steps, _, width = path_ref.shape
    span = steps // CHUNKS
    is_final = lax.axis_index("tm") == lax.axis_size("tm") - 1
    here = lax.axis_index("tm") // PLANE == hop
    column = as_column(jnp.where(here, came_ref[...], enter_ref[...]))
    for chunk in range(CHUNKS):
        entry = entry_ref[chunk]
        start = jnp.sum(entry[:width] * column, axis=0, keepdims=True) + entry[width : width + 1]
        begin = as_column(jnp.broadcast_to(start, (PAD, width)))
        for step in range(chunk * span, (chunk + 1) * span):
            path = path_ref[step, :width]
            filtered_ref[step : step + 1] = (
                jnp.sum(path * begin, axis=0, keepdims=True) + path_ref[step, width : width + 1]
            )
    filtered = filtered_ref[...]
    step_ids = lax.broadcasted_iota(jnp.int32, (steps, 1), 0)
    keep = jnp.where(jnp.logical_and(step_ids == steps - 1, is_final), 0.0, 1.0)
    change = filtered - keep * dot_split(filtered, mix_ref[...])
    local_ref[...] = suffix_scan(change, high_ref, low_ref, 0, levels)


def smooth_kernel(all_ref, local_ref, high_ref, low_ref, out_ref, sum_ref, *, levels):
    count, width = all_ref.shape
    steps = local_ref.shape[0]
    me = lax.axis_index("tm")
    sum_ref[pl.ds(count, PAD), :] = jnp.zeros((PAD, width), f32)
    sum_ref[pl.ds(0, count), :] = suffix_scan(
        all_ref[...], high_ref, low_ref, levels, (count - 1).bit_length()
    )
    incoming = jnp.broadcast_to(sum_ref[pl.ds(me + 1, 1), :], (PAD, width))
    lifted = dot_few(incoming, high_ref[0], low_ref[0])[0:1]
    step_ids = lax.broadcasted_iota(jnp.int32, (steps, 1), 0)
    rows = jnp.where(step_ids == steps - 1, lifted, 0.0)
    out_ref[...] = local_ref[...] + suffix_scan(rows, high_ref, low_ref, 0, levels)


def call(kernel, outs, scratch=(), flops=0, limit=8, spaces=None):
    extra = {} if spaces is None else {"in_specs": [pl.BlockSpec(memory_space=s) for s in spaces]}
    return pl.pallas_call(
        kernel,
        out_shape=outs,
        **extra,
        scratch_shapes=scratch,
        compiler_params=pltpu.CompilerParams(vmem_limit_bytes=limit << 20),
        cost_estimate=pl.CostEstimate(flops=flops, bytes_accessed=1 << 20, transcendentals=0),
    )


def swap(count, distance):
    return [(index, index ^ distance) for index in range(count)]


def per_device(
    observations, obs_weights, damping, transition, obs_matrix, smoother_gain, prior_mean
):
    observations, obs_weights, damping, transition, obs_matrix, smoother_gain, prior_row = (
        pltpu.with_memory_space_constraint(value, pltpu.HBM)
        for value in (
            observations, obs_weights, damping, transition, obs_matrix, smoother_gain,
            prior_mean[None, :],
        )
    )
    steps, width = damping.shape
    count = lax.axis_size("tm")
    rows = width + PAD
    levels = (steps - 1).bit_length()
    cube = 2 * width**3

    def struct(*shape, dtype=f32):
        return jax.ShapeDtypeStruct(shape, dtype)

    path, chunk_maps, total = call(
        local_kernel,
        (struct(steps, rows, width), struct(CHUNKS - 1, rows, width), struct(rows, width)),
        (
            pltpu.VMEM((CHUNKS, width, width), bf16),
            pltpu.VMEM((CHUNKS, width, width), bf16),
            pltpu.VMEM((CHUNKS, width, width), bf16),
            pltpu.VMEM((CHUNKS, width, width), bf16),
            pltpu.VMEM((CHUNKS, rows, width), f32),
            pltpu.VMEM((steps, width), f32),
            pltpu.VMEM((steps, width), f32),
            pltpu.VMEM((2, width, width), f32),
            pltpu.VMEM(observations.shape, f32),
            pltpu.VMEM(obs_weights.shape, f32),
            pltpu.VMEM(damping.shape, f32),
            pltpu.VMEM(transition.shape, f32),
            pltpu.VMEM(obs_matrix.shape, f32),
            pltpu.VMEM((1, width), f32),
            pltpu.SemaphoreType.DMA((6,)),
        ),
        flops=130 * cube,
        limit=32,
        spaces=[pltpu.HBM] * 6,
    )(observations, obs_weights, damping, transition, obs_matrix, prior_row)

    partner = lax.ppermute(total, "tm", swap(count, 1))
    chip, half = call(
        pair_kernel, (struct(rows, width), struct(rows, width // 2)), flops=3 * cube
    )(total, partner)

    straight = [(index, index ^ (4 if index % 2 else 2)) for index in range(count)]
    diagonal = lax.ppermute(half, "tm", swap(count, 6))
    whole = lax.ppermute(chip, "tm", straight)
    middle = width // 2
    power_count = levels + max((count - 1).bit_length(), 1)
    mix, power_high, power_low = call(
        power_kernel,
        (
            struct(3 * width, width, dtype=bf16),
            struct(power_count, width, width, dtype=bf16),
            struct(power_count, width, width, dtype=bf16),
        ),
        (
            pltpu.VMEM(transition.shape, f32),
            pltpu.VMEM(transition.shape, f32),
            pltpu.SemaphoreType.DMA((2,)),
        ),
        flops=60 * cube,
        spaces=[pltpu.HBM, pltpu.HBM, pl.ANY],
    )(transition, smoother_gain, half)
    whole, diagonal, mix = lax.optimization_barrier((whole, diagonal, mix))
    halves = jnp.stack([whole[:, :middle], whole[:, middle:], diagonal])
    other_halves = lax.ppermute(halves, "tm", swap(count, 1))
    plane, before, leave = call(
        plane_kernel,
        (struct(rows, width), struct(rows, width), struct(PAD, width)),
        (pltpu.VMEM((4, rows, width), f32), pltpu.VMEM((4, rows, width), f32)),
        flops=9 * cube,
        spaces=[pltpu.VMEM] * 3 + [pl.ANY],
    )(chip, halves, other_halves, mix)
    entry = call(entry_kernel, struct(CHUNKS, rows, width), flops=12 * cube)(
        before, partner, chunk_maps
    )

    enter = jnp.zeros((PAD, width), f32)
    came = leave
    hops = count // PLANE - 1
    for hop in range(hops):
        if hop > 0:
            leave, enter = call(
                functools.partial(hop_kernel, hop=hop),
                (struct(PAD, width), struct(PAD, width)),
                flops=cube // 64,
                limit=2,
            )(plane, came, enter)
        low, high = hop * PLANE, (hop + 1) * PLANE
        pairs = [(low + i, high + i) for i in range(PLANE)]
        pairs = pairs + [(b, a) for a, b in pairs]
        came = lax.ppermute(leave, "tm", pairs)

    filtered, local = call(
        functools.partial(filter_kernel, levels=levels, hop=hops),
        (struct(steps, width), struct(steps, width)),
        flops=20 * cube,
    )(came, enter, entry, path, mix, power_high, power_low)

    sent = jnp.broadcast_to(local[0:1], (count, width))
    offsets = lax.all_to_all(sent, "tm", 0, 0, tiled=True)
    smoothed = call(
        functools.partial(smooth_kernel, levels=levels),
        struct(steps, width),
        (pltpu.VMEM((count + PAD, width), f32),),
        flops=20 * cube,
    )(offsets, local, power_high, power_low)
    return filtered, smoothed


def solution(mesh):
    return jax.shard_map(
        per_device,
        mesh=mesh,
        in_specs=(P("tm", None), P("tm", None), P("tm", None), P(), P(), P(), P()),
        out_specs=(P("tm", None), P("tm", None)),
        check_vma=False,
    )
```

```python
import functools

import jax
import jax.numpy as jnp
from jax import lax
from jax.experimental import pallas as pl
from jax.experimental.pallas import tpu as pltpu
from jax.sharding import PartitionSpec as P

f32, bf16 = jnp.float32, jnp.bfloat16
highest = lax.Precision.HIGHEST
PAD = 8
CHUNKS = 4
PLANE = 8


def exact(left, right):
    return jnp.dot(left, right, precision=highest, preferred_element_type=f32)


def split(value):
    high = value.astype(bf16)
    return high, (value - high.astype(f32)).astype(bf16)


def stack_right(high, low):
    return jnp.concatenate([high, low, high], axis=0)


def dot_split(left, right_stack):
    high, low = split(left)
    return jnp.dot(
        jnp.concatenate([high, high, low], axis=1), right_stack, preferred_element_type=f32
    )


def dot_few(left, right_high, right_low):
    count = left.shape[0]
    high, low = split(left)
    stacked = jnp.concatenate(
        [
            jnp.concatenate([high, high], axis=1),
            jnp.concatenate([low, jnp.zeros_like(low)], axis=1),
        ],
        axis=0,
    )
    right = jnp.concatenate([right_high, right_low], axis=0)
    both = jnp.dot(stacked, right, preferred_element_type=f32)
    return both[:count] + both[count:]


def compose(first, second):
    width = first.shape[1]
    joined = dot_split(first, stack_right(*split(second[:width])))
    return jnp.concatenate([joined[:width], joined[width:] + second[width:]], axis=0)


def eye_map(width):
    rows = lax.broadcasted_iota(jnp.int32, (width + PAD, width), 0)
    cols = lax.broadcasted_iota(jnp.int32, (width + PAD, width), 1)
    return (rows == cols).astype(f32)


def as_column(rows):
    return rows.T[:, 0:1]


def fetch(sources, targets, sems):
    copies = [
        pltpu.make_async_copy(source, target, sems.at[index])
        for index, (source, target) in enumerate(zip(sources, targets))
    ]
    for copy in copies:
        copy.start()
    for copy in copies:
        copy.wait()


def local_kernel(
    obs_hbm, weight_hbm, damp_hbm, trans_hbm, obsmat_hbm, prior_hbm,
    path_ref, chunk_ref, total_ref,
    high_even, low_even, high_odd, low_odd, state_ref, offset_ref, wide_ref, base_ref,
    obs_ref, weight_ref, damp_ref, trans_ref, obsmat_ref, prior_ref, sems,
):
    fetch(
        (trans_hbm, obsmat_hbm, damp_hbm, weight_hbm, obs_hbm, prior_hbm),
        (trans_ref, obsmat_ref, damp_ref, weight_ref, obs_ref, prior_ref),
        sems,
    )
    steps, width = damp_ref.shape
    span = steps // CHUNKS
    is_first = (lax.axis_index("tm") == 0).astype(f32)
    obs_mat = obsmat_ref[...]
    weights = weight_ref[...]
    trans_t = trans_ref[...].T
    base_ref[0] = trans_t
    observed = lax.dot_general(
        trans_t, obs_mat, (((1,), (1,)), ((), ())), precision=highest, preferred_element_type=f32
    )
    base_ref[1] = jnp.concatenate([observed] * 4, axis=1)
    wide_ref[...] = jnp.concatenate([weights] * 4, axis=1)
    obs_high, obs_low = split(obs_mat)
    obs_stack = jnp.concatenate([obs_high, obs_low, obs_high, obs_low], axis=0)

    half = width // 2

    def make(time):
        scaled = base_ref[1] * wide_ref[pl.ds(time, 1), :]
        high, low = split(scaled)
        pieces = jnp.concatenate([high[:, :half], low[:, half:]], axis=1)
        return base_ref[0] - jnp.dot(pieces, obs_stack, preferred_element_type=f32)

    for chunk in range(CHUNKS):
        time = chunk * span
        damp = as_column(jnp.broadcast_to(damp_ref[time : time + 1], (PAD, width)))
        begin = make(time) * damp
        if chunk == 0:
            begin = begin * (1.0 - is_first)
        state_ref[chunk, :width] = begin
        path_ref[time, :width] = begin

    def ready(step, chunk, slot):
        slot[0][chunk], slot[1][chunk] = split(make(chunk * span + step))

    def advance(step, slot, following):
        for chunk in range(CHUNKS):
            time = chunk * span + step
            damped = state_ref[chunk] * damp_ref[pl.ds(time, 1), :]
            moved = dot_split(damped, stack_right(slot[0][chunk], slot[1][chunk]))
            moved = jnp.concatenate(
                [moved[:width], moved[width:] + offset_ref[pl.ds(time, 1), :]], axis=0
            )
            state_ref[chunk] = moved
            path_ref[time] = moved
            if following is not None:
                ready(step + 1, chunk, following)

    even, odd = (high_even, low_even), (high_odd, low_odd)
    for chunk in range(CHUNKS):
        ready(1, chunk, odd)

    offsets = exact(weights * obs_ref[...], obs_mat)
    prior = jnp.broadcast_to(prior_ref[...], (PAD, width))
    seen = lax.dot_general(
        prior, obs_mat, (((1,), (1,)), ((), ())), precision=highest, preferred_element_type=f32
    )
    begun = prior - exact(seen * weights[0:1], obs_mat)
    step_ids = lax.broadcasted_iota(jnp.int32, (steps, 1), 0)
    offsets = offsets + jnp.where(step_ids == 0, is_first, 0.0) * begun[0:1]
    offset_ref[...] = offsets
    for chunk in range(CHUNKS):
        time = chunk * span
        begin = jnp.broadcast_to(offsets[time : time + 1], (PAD, width))
        state_ref[chunk, width:] = begin
        path_ref[time, width:] = begin

    def two(index, carry):
        advance(2 * index + 1, odd, even)
        advance(2 * index + 2, even, odd)
        return carry

    lax.fori_loop(0, span // 2 - 1, two, 0)
    advance(span - 1, odd, None)

    first = compose(state_ref[0], state_ref[1])
    chunk_ref[0] = state_ref[0]
    chunk_ref[1] = first
    chunk_ref[2] = state_ref[2]
    total_ref[...] = compose(first, compose(state_ref[2], state_ref[3]))


def pair_kernel(mine_ref, other_ref, chip_ref, half_ref):
    core = lax.axis_index("tm") % 2
    mine, other = mine_ref[...], other_ref[...]
    upper = core == 1
    whole = compose(jnp.where(upper, other, mine), jnp.where(upper, mine, other))
    chip_ref[...] = whole
    half = whole.shape[1] // 2
    half_ref[...] = jnp.where(upper, whole[:, half:], whole[:, :half])


def plane_kernel(
    chip_ref, mine_ref, other_ref, _, plane_ref, before_ref, leave_ref, all_ref, prefix_ref
):
    me = lax.axis_index("tm")
    upper = me % 2 == 1
    place = (me // 2) % 4
    half = chip_ref.shape[1] // 2
    all_ref[place] = chip_ref[...]
    for part in range(2):
        mine, other = mine_ref[part], other_ref[part]
        columns = pl.ds(part * half, half)
        all_ref[place ^ 1, :, columns] = jnp.where(upper, other, mine)
        all_ref[place ^ 2, :, columns] = jnp.where(upper, mine, other)
    mine, other = mine_ref[2], other_ref[2]
    all_ref[place ^ 3, :, :half] = jnp.where(upper, other, mine)
    all_ref[place ^ 3, :, half:] = jnp.where(upper, mine, other)
    width = chip_ref.shape[1]
    left = compose(all_ref[0], all_ref[1])
    right = compose(all_ref[2], all_ref[3])
    whole = compose(left, right)
    plane_ref[...] = whole
    leave_ref[...] = whole[width:]
    prefix_ref[0] = eye_map(width)
    prefix_ref[1] = all_ref[0]
    prefix_ref[2] = left
    prefix_ref[3] = compose(left, all_ref[2])
    before_ref[...] = prefix_ref[place]


def hop_kernel(plane_ref, came_ref, enter_ref, leave_ref, next_ref, *, hop):
    width = plane_ref.shape[1]
    here = lax.axis_index("tm") // PLANE == hop
    enter = jnp.where(here, came_ref[...], enter_ref[...])
    next_ref[...] = enter
    moved = jnp.sum(plane_ref[:width] * as_column(enter), axis=0, keepdims=True)
    leave_ref[...] = moved + plane_ref[width:]


def entry_kernel(before_ref, other_ref, chunk_ref, entry_ref):
    upper = lax.axis_index("tm") % 2 == 1
    before = before_ref[...]
    joined = compose(before, other_ref[...])
    start = jnp.where(upper, joined, before)
    entry_ref[0] = start
    entry_ref[1] = compose(start, chunk_ref[0])
    entry_ref[2] = compose(start, chunk_ref[1])
    entry_ref[3] = compose(entry_ref[2], chunk_ref[2])


def power_kernel(trans_hbm, gain_hbm, _, mix_ref, high_ref, low_ref, trans_ref, gain_ref, sems):
    fetch((trans_hbm, gain_hbm), (trans_ref, gain_ref), sems)
    gain_t = gain_ref[...].T
    mix_high, mix_low = split(exact(trans_ref[...].T, gain_t))
    mix_ref[...] = stack_right(mix_high, mix_low)
    power = gain_t
    for level in range(high_ref.shape[0]):
        high_ref[level], low_ref[level] = split(power)
        if level + 1 < high_ref.shape[0]:
            power = exact(power, power)


def suffix_scan(rows, high_ref, low_ref, first_level, levels):
    count, width = rows.shape
    for level in range(levels):
        distance = 1 << level
        later = jnp.concatenate(
            [rows[distance:], jnp.zeros((distance, width), f32)], axis=0
        )
        rows = rows + dot_few(later, high_ref[first_level + level], low_ref[first_level + level])
    return rows


def filter_kernel(
    came_ref, enter_ref, entry_ref, path_ref, mix_ref, high_ref, low_ref,
    filtered_ref, local_ref, *, levels, hop
):
    steps, _, width = path_ref.shape
    span = steps // CHUNKS
    is_final = lax.axis_index("tm") == lax.axis_size("tm") - 1
    here = lax.axis_index("tm") // PLANE == hop
    column = as_column(jnp.where(here, came_ref[...], enter_ref[...]))
    for chunk in range(CHUNKS):
        entry = entry_ref[chunk]
        start = jnp.sum(entry[:width] * column, axis=0, keepdims=True) + entry[width : width + 1]
        begin = as_column(jnp.broadcast_to(start, (PAD, width)))
        for step in range(chunk * span, (chunk + 1) * span):
            path = path_ref[step, :width]
            filtered_ref[step : step + 1] = (
                jnp.sum(path * begin, axis=0, keepdims=True) + path_ref[step, width : width + 1]
            )
    filtered = filtered_ref[...]
    step_ids = lax.broadcasted_iota(jnp.int32, (steps, 1), 0)
    keep = jnp.where(jnp.logical_and(step_ids == steps - 1, is_final), 0.0, 1.0)
    change = filtered - keep * dot_split(filtered, mix_ref[...])
    local_ref[...] = suffix_scan(change, high_ref, low_ref, 0, levels)


def smooth_kernel(all_ref, local_ref, high_ref, low_ref, out_ref, sum_ref, *, levels):
    count, width = all_ref.shape
    steps = local_ref.shape[0]
    me = lax.axis_index("tm")
    sum_ref[pl.ds(count, PAD), :] = jnp.zeros((PAD, width), f32)
    sum_ref[pl.ds(0, count), :] = suffix_scan(
        all_ref[...], high_ref, low_ref, levels, (count - 1).bit_length()
    )
    incoming = jnp.broadcast_to(sum_ref[pl.ds(me + 1, 1), :], (PAD, width))
    lifted = dot_few(incoming, high_ref[0], low_ref[0])[0:1]
    step_ids = lax.broadcasted_iota(jnp.int32, (steps, 1), 0)
    rows = jnp.where(step_ids == steps - 1, lifted, 0.0)
    out_ref[...] = local_ref[...] + suffix_scan(rows, high_ref, low_ref, 0, levels)


def call(kernel, outs, scratch=(), flops=0, limit=8, spaces=None):
    extra = {} if spaces is None else {"in_specs": [pl.BlockSpec(memory_space=s) for s in spaces]}
    return pl.pallas_call(
        kernel,
        out_shape=outs,
        **extra,
        scratch_shapes=scratch,
        compiler_params=pltpu.CompilerParams(vmem_limit_bytes=limit << 20),
        cost_estimate=pl.CostEstimate(flops=flops, bytes_accessed=1 << 20, transcendentals=0),
    )


def swap(count, distance):
    return [(index, index ^ distance) for index in range(count)]


def per_device(
    observations, obs_weights, damping, transition, obs_matrix, smoother_gain, prior_mean
):
    observations, obs_weights, damping, transition, obs_matrix, smoother_gain, prior_row = (
        pltpu.with_memory_space_constraint(value, pltpu.HBM)
        for value in (
            observations, obs_weights, damping, transition, obs_matrix, smoother_gain,
            prior_mean[None, :],
        )
    )
    steps, width = damping.shape
    count = lax.axis_size("tm")
    rows = width + PAD
    levels = (steps - 1).bit_length()
    cube = 2 * width**3

    def struct(*shape, dtype=f32):
        return jax.ShapeDtypeStruct(shape, dtype)

    path, chunk_maps, total = call(
        local_kernel,
        (struct(steps, rows, width), struct(CHUNKS - 1, rows, width), struct(rows, width)),
        (
            pltpu.VMEM((CHUNKS, width, width), bf16),
            pltpu.VMEM((CHUNKS, width, width), bf16),
            pltpu.VMEM((CHUNKS, width, width), bf16),
            pltpu.VMEM((CHUNKS, width, width), bf16),
            pltpu.VMEM((CHUNKS, rows, width), f32),
            pltpu.VMEM((steps, width), f32),
            pltpu.VMEM((steps, width), f32),
            pltpu.VMEM((2, width, width), f32),
            pltpu.VMEM(observations.shape, f32),
            pltpu.VMEM(obs_weights.shape, f32),
            pltpu.VMEM(damping.shape, f32),
            pltpu.VMEM(transition.shape, f32),
            pltpu.VMEM(obs_matrix.shape, f32),
            pltpu.VMEM((1, width), f32),
            pltpu.SemaphoreType.DMA((6,)),
        ),
        flops=130 * cube,
        limit=32,
        spaces=[pltpu.HBM] * 6,
    )(observations, obs_weights, damping, transition, obs_matrix, prior_row)

    partner = lax.ppermute(total, "tm", swap(count, 1))
    chip, half = call(
        pair_kernel, (struct(rows, width), struct(rows, width // 2)), flops=3 * cube
    )(total, partner)

    straight = [(index, index ^ (4 if index % 2 else 2)) for index in range(count)]
    diagonal = lax.ppermute(half, "tm", swap(count, 6))
    whole = lax.ppermute(chip, "tm", straight)
    middle = width // 2
    power_count = levels + max((count - 1).bit_length(), 1)
    mix, power_high, power_low = call(
        power_kernel,
        (
            struct(3 * width, width, dtype=bf16),
            struct(power_count, width, width, dtype=bf16),
            struct(power_count, width, width, dtype=bf16),
        ),
        (
            pltpu.VMEM(transition.shape, f32),
            pltpu.VMEM(transition.shape, f32),
            pltpu.SemaphoreType.DMA((2,)),
        ),
        flops=60 * cube,
        spaces=[pltpu.HBM, pltpu.HBM, pl.ANY],
    )(transition, smoother_gain, half)
    whole, diagonal, mix = lax.optimization_barrier((whole, diagonal, mix))
    halves = jnp.stack([whole[:, :middle], whole[:, middle:], diagonal])
    other_halves = lax.ppermute(halves, "tm", swap(count, 1))
    plane, before, leave = call(
        plane_kernel,
        (struct(rows, width), struct(rows, width), struct(PAD, width)),
        (pltpu.VMEM((4, rows, width), f32), pltpu.VMEM((4, rows, width), f32)),
        flops=9 * cube,
        spaces=[pltpu.VMEM] * 3 + [pl.ANY],
    )(chip, halves, other_halves, mix)
    entry = call(entry_kernel, struct(CHUNKS, rows, width), flops=12 * cube)(
        before, partner, chunk_maps
    )

    enter = jnp.zeros((PAD, width), f32)
    came = leave
    hops = count // PLANE - 1
    for hop in range(hops):
        if hop > 0:
            leave, enter = call(
                functools.partial(hop_kernel, hop=hop),
                (struct(PAD, width), struct(PAD, width)),
                flops=cube // 64,
                limit=2,
            )(plane, came, enter)
        low, high = hop * PLANE, (hop + 1) * PLANE
        pairs = [(low + i, high + i) for i in range(PLANE)]
        came = lax.ppermute(leave, "tm", pairs)

    filtered, local = call(
        functools.partial(filter_kernel, levels=levels, hop=hops),
        (struct(steps, width), struct(steps, width)),
        flops=20 * cube,
    )(came, enter, entry, path, mix, power_high, power_low)

    sent = jnp.broadcast_to(local[0:1], (count, width))
    offsets = lax.all_to_all(sent, "tm", 0, 0, tiled=True)
    smoothed = call(
        functools.partial(smooth_kernel, levels=levels),
        struct(steps, width),
        (pltpu.VMEM((count + PAD, width), f32),),
        flops=20 * cube,
    )(offsets, local, power_high, power_low)
    return filtered, smoothed


def solution(mesh):
    return jax.shard_map(
        per_device,
        mesh=mesh,
        in_specs=(P("tm", None), P("tm", None), P("tm", None), P(), P(), P(), P()),
        out_specs=(P("tm", None), P("tm", None)),
        check_vma=False,
    )
```

```python
import functools

import jax
import jax.numpy as jnp
from jax import lax
from jax.experimental import pallas as pl
from jax.experimental.pallas import tpu as pltpu
from jax.sharding import PartitionSpec as P

f32, bf16 = jnp.float32, jnp.bfloat16
highest = lax.Precision.HIGHEST
PAD = 8
CHUNKS = 4
PLANE = 8


def exact(left, right):
    return jnp.dot(left, right, precision=highest, preferred_element_type=f32)


def split(value):
    high = value.astype(bf16)
    return high, (value - high.astype(f32)).astype(bf16)


def stack_right(high, low):
    return jnp.concatenate([high, low, high], axis=0)


def dot_split(left, right_stack):
    high, low = split(left)
    return jnp.dot(
        jnp.concatenate([high, high, low], axis=1), right_stack, preferred_element_type=f32
    )


def dot_few(left, right_high, right_low):
    count = left.shape[0]
    high, low = split(left)
    stacked = jnp.concatenate(
        [
            jnp.concatenate([high, high], axis=1),
            jnp.concatenate([low, jnp.zeros_like(low)], axis=1),
        ],
        axis=0,
    )
    right = jnp.concatenate([right_high, right_low], axis=0)
    both = jnp.dot(stacked, right, preferred_element_type=f32)
    return both[:count] + both[count:]


def compose(first, second):
    width = first.shape[1]
    joined = dot_split(first, stack_right(*split(second[:width])))
    return jnp.concatenate([joined[:width], joined[width:] + second[width:]], axis=0)


def eye_map(width):
    rows = lax.broadcasted_iota(jnp.int32, (width + PAD, width), 0)
    cols = lax.broadcasted_iota(jnp.int32, (width + PAD, width), 1)
    return (rows == cols).astype(f32)


def as_column(rows):
    return rows.T[:, 0:1]


def fetch(sources, targets, sems):
    copies = [
        pltpu.make_async_copy(source, target, sems.at[index])
        for index, (source, target) in enumerate(zip(sources, targets))
    ]
    for copy in copies:
        copy.start()
    for copy in copies:
        copy.wait()


def local_kernel(
    obs_hbm, weight_hbm, damp_hbm, trans_hbm, obsmat_hbm, prior_hbm,
    path_ref, chunk_ref, total_ref,
    high_even, low_even, high_odd, low_odd, state_ref, offset_ref, wide_ref, base_ref,
    obs_ref, weight_ref, damp_ref, trans_ref, obsmat_ref, prior_ref, sems,
):
    fetch(
        (trans_hbm, obsmat_hbm, damp_hbm, weight_hbm, obs_hbm, prior_hbm),
        (trans_ref, obsmat_ref, damp_ref, weight_ref, obs_ref, prior_ref),
        sems,
    )
    steps, width = damp_ref.shape
    span = steps // CHUNKS
    is_first = (lax.axis_index("tm") == 0).astype(f32)
    obs_mat = obsmat_ref[...]
    weights = weight_ref[...]
    trans_t = trans_ref[...].T
    base_ref[0] = trans_t
    observed = lax.dot_general(
        trans_t, obs_mat, (((1,), (1,)), ((), ())), precision=highest, preferred_element_type=f32
    )
    base_ref[1] = jnp.concatenate([observed] * 4, axis=1)
    wide_ref[...] = jnp.concatenate([weights] * 4, axis=1)
    obs_high, obs_low = split(obs_mat)
    obs_stack = jnp.concatenate([obs_high, obs_low, obs_high, obs_low], axis=0)

    half = width // 2

    def make(time):
        scaled = base_ref[1] * wide_ref[pl.ds(time, 1), :]
        high, low = split(scaled)
        pieces = jnp.concatenate([high[:, :half], low[:, half:]], axis=1)
        return base_ref[0] - jnp.dot(pieces, obs_stack, preferred_element_type=f32)

    for chunk in range(CHUNKS):
        time = chunk * span
        damp = as_column(jnp.broadcast_to(damp_ref[time : time + 1], (PAD, width)))
        begin = make(time) * damp
        if chunk == 0:
            begin = begin * (1.0 - is_first)
        state_ref[chunk, :width] = begin
        path_ref[time, :width] = begin

    def ready(step, chunk, slot):
        slot[0][chunk], slot[1][chunk] = split(make(chunk * span + step))

    def advance(step, slot, following):
        for chunk in range(CHUNKS):
            time = chunk * span + step
            damped = state_ref[chunk] * damp_ref[pl.ds(time, 1), :]
            moved = dot_split(damped, stack_right(slot[0][chunk], slot[1][chunk]))
            moved = jnp.concatenate(
                [moved[:width], moved[width:] + offset_ref[pl.ds(time, 1), :]], axis=0
            )
            state_ref[chunk] = moved
            path_ref[time] = moved
            if following is not None:
                ready(step + 1, chunk, following)

    even, odd = (high_even, low_even), (high_odd, low_odd)
    for chunk in range(CHUNKS):
        ready(1, chunk, odd)

    offsets = exact(weights * obs_ref[...], obs_mat)
    prior = jnp.broadcast_to(prior_ref[...], (PAD, width))
    seen = lax.dot_general(
        prior, obs_mat, (((1,), (1,)), ((), ())), precision=highest, preferred_element_type=f32
    )
    begun = prior - exact(seen * weights[0:1], obs_mat)
    step_ids = lax.broadcasted_iota(jnp.int32, (steps, 1), 0)
    offsets = offsets + jnp.where(step_ids == 0, is_first, 0.0) * begun[0:1]
    offset_ref[...] = offsets
    for chunk in range(CHUNKS):
        time = chunk * span
        begin = jnp.broadcast_to(offsets[time : time + 1], (PAD, width))
        state_ref[chunk, width:] = begin
        path_ref[time, width:] = begin

    def two(index, carry):
        advance(2 * index + 1, odd, even)
        advance(2 * index + 2, even, odd)
        return carry

    lax.fori_loop(0, span // 2 - 1, two, 0)
    advance(span - 1, odd, None)

    first = compose(state_ref[0], state_ref[1])
    chunk_ref[0] = state_ref[0]
    chunk_ref[1] = first
    chunk_ref[2] = state_ref[2]
    total_ref[...] = compose(first, compose(state_ref[2], state_ref[3]))


def pair_kernel(mine_ref, other_ref, chip_ref, half_ref):
    core = lax.axis_index("tm") % 2
    mine, other = mine_ref[...], other_ref[...]
    upper = core == 1
    whole = compose(jnp.where(upper, other, mine), jnp.where(upper, mine, other))
    chip_ref[...] = whole
    half = whole.shape[1] // 2
    half_ref[...] = jnp.where(upper, whole[:, half:], whole[:, :half])


def plane_kernel(
    chip_ref, mine_ref, other_ref, _, plane_ref, before_ref, leave_ref, all_ref, prefix_ref
):
    me = lax.axis_index("tm")
    upper = me % 2 == 1
    place = (me // 2) % 4
    half = chip_ref.shape[1] // 2
    all_ref[place] = chip_ref[...]
    for part in range(2):
        mine, other = mine_ref[part], other_ref[part]
        columns = pl.ds(part * half, half)
        all_ref[place ^ 1, :, columns] = jnp.where(upper, other, mine)
        all_ref[place ^ 2, :, columns] = jnp.where(upper, mine, other)
    mine, other = mine_ref[2], other_ref[2]
    all_ref[place ^ 3, :, :half] = jnp.where(upper, other, mine)
    all_ref[place ^ 3, :, half:] = jnp.where(upper, mine, other)
    width = chip_ref.shape[1]
    left = compose(all_ref[0], all_ref[1])
    right = compose(all_ref[2], all_ref[3])
    whole = compose(left, right)
    plane_ref[...] = whole
    leave_ref[...] = whole[width:]
    prefix_ref[0] = eye_map(width)
    prefix_ref[1] = all_ref[0]
    prefix_ref[2] = left
    prefix_ref[3] = compose(left, all_ref[2])
    before_ref[...] = prefix_ref[place]


def hop_kernel(plane_ref, came_ref, enter_ref, leave_ref, next_ref, *, hop):
    width = plane_ref.shape[1]
    here = lax.axis_index("tm") // PLANE == hop
    enter = jnp.where(here, came_ref[...], enter_ref[...])
    next_ref[...] = enter
    moved = jnp.sum(plane_ref[:width] * as_column(enter), axis=0, keepdims=True)
    leave_ref[...] = moved + plane_ref[width:]


def entry_kernel(before_ref, other_ref, chunk_ref, entry_ref):
    upper = lax.axis_index("tm") % 2 == 1
    before = before_ref[...]
    joined = compose(before, other_ref[...])
    start = jnp.where(upper, joined, before)
    entry_ref[0] = start
    entry_ref[1] = compose(start, chunk_ref[0])
    entry_ref[2] = compose(start, chunk_ref[1])
    entry_ref[3] = compose(entry_ref[2], chunk_ref[2])


def power_kernel(trans_hbm, gain_hbm, _, mix_ref, high_ref, low_ref, trans_ref, gain_ref, sems):
    fetch((trans_hbm, gain_hbm), (trans_ref, gain_ref), sems)
    gain_t = gain_ref[...].T
    mix_ref[0], mix_ref[1] = split(exact(trans_ref[...].T, gain_t))
    power = gain_t
    for level in range(high_ref.shape[0]):
        high_ref[level], low_ref[level] = split(power)
        if level + 1 < high_ref.shape[0]:
            power = exact(power, power)


def suffix_scan(rows, high_ref, low_ref, first_level, levels):
    count, width = rows.shape
    for level in range(levels):
        distance = 1 << level
        later = jnp.concatenate(
            [rows[distance:], jnp.zeros((distance, width), f32)], axis=0
        )
        rows = rows + dot_few(later, high_ref[first_level + level], low_ref[first_level + level])
    return rows


def filter_kernel(
    came_ref, enter_ref, came_zero_ref, enter_zero_ref, entry_ref, path_ref, mix_ref, high_ref, low_ref,
    filtered_ref, local_ref, *, levels, hop
):
    steps, _, width = path_ref.shape
    span = steps // CHUNKS
    is_final = lax.axis_index("tm") == lax.axis_size("tm") - 1
    me = lax.axis_index("tm")
    here, upper = me // PLANE == hop, me % 2 == 1
    came = jnp.where(upper, came_ref[...], came_zero_ref[...])
    enter = jnp.where(upper, enter_ref[...], enter_zero_ref[...])
    column = as_column(jnp.where(here, came, enter))
    for chunk in range(CHUNKS):
        entry = entry_ref[chunk]
        start = jnp.sum(entry[:width] * column, axis=0, keepdims=True) + entry[width : width + 1]
        begin = as_column(jnp.broadcast_to(start, (PAD, width)))
        for step in range(chunk * span, (chunk + 1) * span):
            path = path_ref[step, :width]
            filtered_ref[step : step + 1] = (
                jnp.sum(path * begin, axis=0, keepdims=True) + path_ref[step, width : width + 1]
            )
    filtered = filtered_ref[...]
    step_ids = lax.broadcasted_iota(jnp.int32, (steps, 1), 0)
    keep = jnp.where(jnp.logical_and(step_ids == steps - 1, is_final), 0.0, 1.0)
    change = filtered - keep * dot_few(filtered, mix_ref[0], mix_ref[1])
    local_ref[...] = suffix_scan(change, high_ref, low_ref, 0, levels)


def smooth_kernel(all_ref, local_ref, high_ref, low_ref, out_ref, sum_ref, *, levels):
    count, width = all_ref.shape
    steps = local_ref.shape[0]
    me = lax.axis_index("tm")
    sum_ref[pl.ds(count, PAD), :] = jnp.zeros((PAD, width), f32)
    sum_ref[pl.ds(0, count), :] = suffix_scan(
        all_ref[...], high_ref, low_ref, levels, (count - 1).bit_length()
    )
    incoming = jnp.broadcast_to(sum_ref[pl.ds(me + 1, 1), :], (PAD, width))
    lifted = dot_few(incoming, high_ref[0], low_ref[0])[0:1]
    step_ids = lax.broadcasted_iota(jnp.int32, (steps, 1), 0)
    rows = jnp.where(step_ids == steps - 1, lifted, 0.0)
    out_ref[...] = local_ref[...] + suffix_scan(rows, high_ref, low_ref, 0, levels)


def call(kernel, outs, scratch=(), flops=0, limit=8, spaces=None):
    extra = {} if spaces is None else {"in_specs": [pl.BlockSpec(memory_space=s) for s in spaces]}
    return pl.pallas_call(
        kernel,
        out_shape=outs,
        **extra,
        scratch_shapes=scratch,
        compiler_params=pltpu.CompilerParams(vmem_limit_bytes=limit << 20),
        cost_estimate=pl.CostEstimate(flops=flops, bytes_accessed=1 << 20, transcendentals=0),
    )


def swap(count, distance):
    return [(index, index ^ distance) for index in range(count)]


def per_device(
    observations, obs_weights, damping, transition, obs_matrix, smoother_gain, prior_mean
):
    observations, obs_weights, damping, transition, obs_matrix, smoother_gain, prior_row = (
        pltpu.with_memory_space_constraint(value, pltpu.HBM)
        for value in (
            observations, obs_weights, damping, transition, obs_matrix, smoother_gain,
            prior_mean[None, :],
        )
    )
    steps, width = damping.shape
    count = lax.axis_size("tm")
    rows = width + PAD
    levels = (steps - 1).bit_length()
    cube = 2 * width**3

    def struct(*shape, dtype=f32):
        return jax.ShapeDtypeStruct(shape, dtype)

    path, chunk_maps, total = call(
        local_kernel,
        (struct(steps, rows, width), struct(CHUNKS - 1, rows, width), struct(rows, width)),
        (
            pltpu.VMEM((CHUNKS, width, width), bf16),
            pltpu.VMEM((CHUNKS, width, width), bf16),
            pltpu.VMEM((CHUNKS, width, width), bf16),
            pltpu.VMEM((CHUNKS, width, width), bf16),
            pltpu.VMEM((CHUNKS, rows, width), f32),
            pltpu.VMEM((steps, width), f32),
            pltpu.VMEM((steps, width), f32),
            pltpu.VMEM((2, width, width), f32),
            pltpu.VMEM(observations.shape, f32),
            pltpu.VMEM(obs_weights.shape, f32),
            pltpu.VMEM(damping.shape, f32),
            pltpu.VMEM(transition.shape, f32),
            pltpu.VMEM(obs_matrix.shape, f32),
            pltpu.VMEM((1, width), f32),
            pltpu.SemaphoreType.DMA((6,)),
        ),
        flops=130 * cube,
        limit=32,
        spaces=[pltpu.HBM] * 6,
    )(observations, obs_weights, damping, transition, obs_matrix, prior_row)

    partner = lax.ppermute(total, "tm", swap(count, 1))
    chip, half = call(
        pair_kernel, (struct(rows, width), struct(rows, width // 2)), flops=3 * cube
    )(total, partner)

    straight = [(index, index ^ (4 if index % 2 else 2)) for index in range(count)]
    diagonal = lax.ppermute(half, "tm", swap(count, 6))
    whole = lax.ppermute(chip, "tm", straight)
    middle = width // 2
    power_count = levels + max((count - 1).bit_length(), 1)
    mix, power_high, power_low = call(
        power_kernel,
        (
            struct(2, width, width, dtype=bf16),
            struct(power_count, width, width, dtype=bf16),
            struct(power_count, width, width, dtype=bf16),
        ),
        (
            pltpu.VMEM(transition.shape, f32),
            pltpu.VMEM(transition.shape, f32),
            pltpu.SemaphoreType.DMA((2,)),
        ),
        flops=60 * cube,
        spaces=[pltpu.HBM, pltpu.HBM, pl.ANY],
    )(transition, smoother_gain, half)
    whole, diagonal, mix = lax.optimization_barrier((whole, diagonal, mix))
    halves = jnp.stack([whole[:, :middle], whole[:, middle:], diagonal])
    other_halves = lax.ppermute(halves, "tm", swap(count, 1))
    plane, before, leave = call(
        plane_kernel,
        (struct(rows, width), struct(rows, width), struct(PAD, width)),
        (pltpu.VMEM((4, rows, width), f32), pltpu.VMEM((4, rows, width), f32)),
        flops=9 * cube,
        spaces=[pltpu.VMEM] * 3 + [pl.ANY],
    )(chip, halves, other_halves, mix)
    entry = call(entry_kernel, struct(CHUNKS, rows, width), flops=12 * cube)(
        before, partner, chunk_maps
    )

    enter = jnp.zeros((PAD, width), f32)
    came = enter
    hops = count // PLANE - 1
    for hop in range(hops):
        if hop > 0:
            leave, enter = call(
                functools.partial(hop_kernel, hop=hop),
                (struct(PAD, width), struct(PAD, width)),
                flops=cube // 64,
                limit=2,
            )(plane, came, enter)
        low, high = hop * PLANE, (hop + 1) * PLANE
        pairs = [(low + i, high + i) for i in range(1, PLANE, 2)]
        came = lax.ppermute(leave, "tm", pairs)

    to_zero = [(index, index - 1) for index in range(1, count, 2)]
    enter_zero = lax.ppermute(enter, "tm", to_zero)
    came, entry = lax.optimization_barrier((came, entry))
    came_zero = lax.ppermute(came, "tm", to_zero)
    filtered, local = call(
        functools.partial(filter_kernel, levels=levels, hop=hops),
        (struct(steps, width), struct(steps, width)),
        flops=20 * cube,
    )(came, enter, came_zero, enter_zero, entry, path, mix, power_high, power_low)

    sent = jnp.broadcast_to(local[0:1], (count, width))
    offsets = lax.all_to_all(sent, "tm", 0, 0, tiled=True)
    smoothed = call(
        functools.partial(smooth_kernel, levels=levels),
        struct(steps, width),
        (pltpu.VMEM((count + PAD, width), f32),),
        flops=20 * cube,
    )(offsets, local, power_high, power_low)
    return filtered, smoothed


def solution(mesh):
    return jax.shard_map(
        per_device,
        mesh=mesh,
        in_specs=(P("tm", None), P("tm", None), P("tm", None), P(), P(), P(), P()),
        out_specs=(P("tm", None), P("tm", None)),
        check_vma=False,
    )
```

```python
import functools

import jax
import jax.numpy as jnp
from jax import lax
from jax.experimental import pallas as pl
from jax.experimental.pallas import tpu as pltpu
from jax.sharding import PartitionSpec as P

f32, bf16 = jnp.float32, jnp.bfloat16
highest = lax.Precision.HIGHEST
PAD = 8
CHUNKS = 4
PLANE = 8


def exact(left, right):
    return jnp.dot(left, right, precision=highest, preferred_element_type=f32)


def split(value):
    high = value.astype(bf16)
    return high, (value - high.astype(f32)).astype(bf16)


def stack_right(high, low):
    return jnp.concatenate([high, low, high], axis=0)


def dot_split(left, right_stack):
    high, low = split(left)
    return jnp.dot(
        jnp.concatenate([high, high, low], axis=1), right_stack, preferred_element_type=f32
    )


def dot_few(left, right_high, right_low):
    count = left.shape[0]
    high, low = split(left)
    stacked = jnp.concatenate(
        [
            jnp.concatenate([high, high], axis=1),
            jnp.concatenate([low, jnp.zeros_like(low)], axis=1),
        ],
        axis=0,
    )
    right = jnp.concatenate([right_high, right_low], axis=0)
    both = jnp.dot(stacked, right, preferred_element_type=f32)
    return both[:count] + both[count:]


def compose(first, second):
    width = first.shape[1]
    joined = dot_split(first, stack_right(*split(second[:width])))
    return jnp.concatenate([joined[:width], joined[width:] + second[width:]], axis=0)


def eye_map(width):
    rows = lax.broadcasted_iota(jnp.int32, (width + PAD, width), 0)
    cols = lax.broadcasted_iota(jnp.int32, (width + PAD, width), 1)
    return (rows == cols).astype(f32)


def as_column(rows):
    return rows.T[:, 0:1]


def fetch(sources, targets, sems):
    copies = [
        pltpu.make_async_copy(source, target, sems.at[index])
        for index, (source, target) in enumerate(zip(sources, targets))
    ]
    for copy in copies:
        copy.start()
    for copy in copies:
        copy.wait()


def local_kernel(
    obs_hbm, weight_hbm, damp_hbm, trans_hbm, obsmat_hbm, prior_hbm,
    path_ref, chunk_ref, total_ref,
    high_even, low_even, high_odd, low_odd, state_ref, offset_ref, wide_ref, base_ref,
    obs_ref, weight_ref, damp_ref, trans_ref, obsmat_ref, prior_ref, sems,
):
    fetch(
        (trans_hbm, obsmat_hbm, damp_hbm, weight_hbm, obs_hbm, prior_hbm),
        (trans_ref, obsmat_ref, damp_ref, weight_ref, obs_ref, prior_ref),
        sems,
    )
    steps, width = damp_ref.shape
    span = steps // CHUNKS
    is_first = (lax.axis_index("tm") == 0).astype(f32)
    obs_mat = obsmat_ref[...]
    weights = weight_ref[...]
    trans_t = trans_ref[...].T
    base_ref[0] = trans_t
    observed = lax.dot_general(
        trans_t, obs_mat, (((1,), (1,)), ((), ())), precision=highest, preferred_element_type=f32
    )
    base_ref[1] = jnp.concatenate([observed] * 4, axis=1)
    wide_ref[...] = jnp.concatenate([weights] * 4, axis=1)
    obs_high, obs_low = split(obs_mat)
    obs_stack = jnp.concatenate([obs_high, obs_low, obs_high, obs_low], axis=0)

    half = width // 2

    def make(time):
        scaled = base_ref[1] * wide_ref[pl.ds(time, 1), :]
        high, low = split(scaled)
        pieces = jnp.concatenate([high[:, :half], low[:, half:]], axis=1)
        return base_ref[0] - jnp.dot(pieces, obs_stack, preferred_element_type=f32)

    for chunk in range(CHUNKS):
        time = chunk * span
        damp = as_column(jnp.broadcast_to(damp_ref[time : time + 1], (PAD, width)))
        begin = make(time) * damp
        if chunk == 0:
            begin = begin * (1.0 - is_first)
        state_ref[chunk, :width] = begin
        path_ref[time, :width] = begin

    def ready(step, chunk, slot):
        slot[0][chunk], slot[1][chunk] = split(make(chunk * span + step))

    def advance(step, slot, following):
        for chunk in range(CHUNKS):
            time = chunk * span + step
            damped = state_ref[chunk] * damp_ref[pl.ds(time, 1), :]
            moved = dot_split(damped, stack_right(slot[0][chunk], slot[1][chunk]))
            moved = jnp.concatenate(
                [moved[:width], moved[width:] + offset_ref[pl.ds(time, 1), :]], axis=0
            )
            state_ref[chunk] = moved
            path_ref[time] = moved
            if following is not None:
                ready(step + 1, chunk, following)

    even, odd = (high_even, low_even), (high_odd, low_odd)
    for chunk in range(CHUNKS):
        ready(1, chunk, odd)

    offsets = exact(weights * obs_ref[...], obs_mat)
    prior = jnp.broadcast_to(prior_ref[...], (PAD, width))
    seen = lax.dot_general(
        prior, obs_mat, (((1,), (1,)), ((), ())), precision=highest, preferred_element_type=f32
    )
    begun = prior - exact(seen * weights[0:1], obs_mat)
    step_ids = lax.broadcasted_iota(jnp.int32, (steps, 1), 0)
    offsets = offsets + jnp.where(step_ids == 0, is_first, 0.0) * begun[0:1]
    offset_ref[...] = offsets
    for chunk in range(CHUNKS):
        time = chunk * span
        begin = jnp.broadcast_to(offsets[time : time + 1], (PAD, width))
        state_ref[chunk, width:] = begin
        path_ref[time, width:] = begin

    def two(index, carry):
        advance(2 * index + 1, odd, even)
        advance(2 * index + 2, even, odd)
        return carry

    lax.fori_loop(0, span // 2 - 1, two, 0)
    advance(span - 1, odd, None)

    first = compose(state_ref[0], state_ref[1])
    chunk_ref[0] = state_ref[0]
    chunk_ref[1] = first
    chunk_ref[2] = state_ref[2]
    total_ref[...] = compose(first, compose(state_ref[2], state_ref[3]))


def pair_kernel(mine_ref, other_ref, chip_ref, half_ref):
    core = lax.axis_index("tm") % 2
    mine, other = mine_ref[...], other_ref[...]
    upper = core == 1
    whole = compose(jnp.where(upper, other, mine), jnp.where(upper, mine, other))
    chip_ref[...] = whole
    half = whole.shape[1] // 2
    half_ref[...] = jnp.where(upper, whole[:, half:], whole[:, :half])


def plane_kernel(
    chip_ref, mine_ref, other_ref, _, plane_ref, before_ref, leave_ref, all_ref, prefix_ref
):
    me = lax.axis_index("tm")
    upper = me % 2 == 1
    place = (me // 2) % 4
    half = chip_ref.shape[1] // 2
    all_ref[place] = chip_ref[...]
    for part in range(2):
        mine, other = mine_ref[part], other_ref[part]
        columns = pl.ds(part * half, half)
        all_ref[place ^ 1, :, columns] = jnp.where(upper, other, mine)
        all_ref[place ^ 2, :, columns] = jnp.where(upper, mine, other)
    mine, other = mine_ref[2], other_ref[2]
    all_ref[place ^ 3, :, :half] = jnp.where(upper, other, mine)
    all_ref[place ^ 3, :, half:] = jnp.where(upper, mine, other)
    width = chip_ref.shape[1]
    left = compose(all_ref[0], all_ref[1])
    right = compose(all_ref[2], all_ref[3])
    whole = compose(left, right)
    plane_ref[...] = whole
    leave_ref[...] = whole[width:]
    prefix_ref[0] = eye_map(width)
    prefix_ref[1] = all_ref[0]
    prefix_ref[2] = left
    prefix_ref[3] = compose(left, all_ref[2])
    before_ref[...] = prefix_ref[place]


def hop_kernel(plane_ref, came_ref, enter_ref, leave_ref, next_ref, *, hop):
    width = plane_ref.shape[1]
    here = lax.axis_index("tm") // PLANE == hop
    enter = jnp.where(here, came_ref[...], enter_ref[...])
    next_ref[...] = enter
    moved = jnp.sum(plane_ref[:width] * as_column(enter), axis=0, keepdims=True)
    leave_ref[...] = moved + plane_ref[width:]


def entry_kernel(before_ref, other_ref, chunk_ref, entry_ref):
    upper = lax.axis_index("tm") % 2 == 1
    before = before_ref[...]
    joined = compose(before, other_ref[...])
    start = jnp.where(upper, joined, before)
    entry_ref[0] = start
    entry_ref[1] = compose(start, chunk_ref[0])
    entry_ref[2] = compose(start, chunk_ref[1])
    entry_ref[3] = compose(entry_ref[2], chunk_ref[2])


def power_kernel(trans_hbm, gain_hbm, _, mix_ref, high_ref, low_ref, trans_ref, gain_ref, sems):
    fetch((trans_hbm, gain_hbm), (trans_ref, gain_ref), sems)
    gain_t = gain_ref[...].T
    mix_ref[0], mix_ref[1] = split(exact(trans_ref[...].T, gain_t))
    power = gain_t
    for level in range(high_ref.shape[0]):
        high_ref[level], low_ref[level] = split(power)
        if level + 1 < high_ref.shape[0]:
            power = exact(power, power)


def suffix_scan(rows, high_ref, low_ref, first_level, levels):
    count, width = rows.shape
    for level in range(levels):
        distance = 1 << level
        later = jnp.concatenate(
            [rows[distance:], jnp.zeros((distance, width), f32)], axis=0
        )
        rows = rows + dot_few(later, high_ref[first_level + level], low_ref[first_level + level])
    return rows


def filter_kernel(
    came_ref, enter_ref, came_zero_ref, enter_zero_ref, entry_ref, path_ref, mix_ref, high_ref, low_ref,
    filtered_ref, local_ref, *, levels, hop
):
    steps, _, width = path_ref.shape
    span = steps // CHUNKS
    is_final = lax.axis_index("tm") == lax.axis_size("tm") - 1
    me = lax.axis_index("tm")
    here, upper = me // PLANE == hop, me % 2 == 1
    came = jnp.where(upper, came_ref[...], came_zero_ref[...])
    enter = jnp.where(upper, enter_ref[...], enter_zero_ref[...])
    column = as_column(jnp.where(here, came, enter))
    for chunk in range(CHUNKS):
        entry = entry_ref[chunk]
        start = jnp.sum(entry[:width] * column, axis=0, keepdims=True) + entry[width : width + 1]
        begin = as_column(jnp.broadcast_to(start, (PAD, width)))
        for step in range(chunk * span, (chunk + 1) * span):
            path = path_ref[step, :width]
            filtered_ref[step : step + 1] = (
                jnp.sum(path * begin, axis=0, keepdims=True) + path_ref[step, width : width + 1]
            )
    filtered = filtered_ref[...]
    step_ids = lax.broadcasted_iota(jnp.int32, (steps, 1), 0)
    keep = jnp.where(jnp.logical_and(step_ids == steps - 1, is_final), 0.0, 1.0)
    change = filtered - keep * dot_few(filtered, mix_ref[0], mix_ref[1])
    local_ref[...] = suffix_scan(change, high_ref, low_ref, 0, levels)


def smooth_kernel(all_ref, local_ref, high_ref, low_ref, out_ref, sum_ref, *, levels):
    count, width = all_ref.shape
    steps = local_ref.shape[0]
    me = lax.axis_index("tm")
    sum_ref[pl.ds(count, PAD), :] = jnp.zeros((PAD, width), f32)
    sum_ref[pl.ds(0, count), :] = suffix_scan(
        all_ref[...], high_ref, low_ref, levels, (count - 1).bit_length()
    )
    incoming = jnp.broadcast_to(sum_ref[pl.ds(me + 1, 1), :], (PAD, width))
    lifted = dot_few(incoming, high_ref[0], low_ref[0])[0:1]
    step_ids = lax.broadcasted_iota(jnp.int32, (steps, 1), 0)
    rows = jnp.where(step_ids == steps - 1, lifted, 0.0)
    out_ref[...] = local_ref[...] + suffix_scan(rows, high_ref, low_ref, 0, levels)


def call(kernel, outs, scratch=(), flops=0, limit=8, spaces=None):
    extra = {} if spaces is None else {"in_specs": [pl.BlockSpec(memory_space=s) for s in spaces]}
    return pl.pallas_call(
        kernel,
        out_shape=outs,
        **extra,
        scratch_shapes=scratch,
        compiler_params=pltpu.CompilerParams(vmem_limit_bytes=limit << 20),
        cost_estimate=pl.CostEstimate(flops=flops, bytes_accessed=1 << 20, transcendentals=0),
    )


def swap(count, distance):
    return [(index, index ^ distance) for index in range(count)]


def per_device(
    observations, obs_weights, damping, transition, obs_matrix, smoother_gain, prior_mean
):
    observations, obs_weights, damping, transition, obs_matrix, smoother_gain, prior_row = (
        pltpu.with_memory_space_constraint(value, pltpu.HBM)
        for value in (
            observations, obs_weights, damping, transition, obs_matrix, smoother_gain,
            prior_mean[None, :],
        )
    )
    steps, width = damping.shape
    count = lax.axis_size("tm")
    rows = width + PAD
    levels = (steps - 1).bit_length()
    cube = 2 * width**3

    def struct(*shape, dtype=f32):
        return jax.ShapeDtypeStruct(shape, dtype)

    path, chunk_maps, total = call(
        local_kernel,
        (struct(steps, rows, width), struct(CHUNKS - 1, rows, width), struct(rows, width)),
        (
            pltpu.VMEM((CHUNKS, width, width), bf16),
            pltpu.VMEM((CHUNKS, width, width), bf16),
            pltpu.VMEM((CHUNKS, width, width), bf16),
            pltpu.VMEM((CHUNKS, width, width), bf16),
            pltpu.VMEM((CHUNKS, rows, width), f32),
            pltpu.VMEM((steps, width), f32),
            pltpu.VMEM((steps, width), f32),
            pltpu.VMEM((2, width, width), f32),
            pltpu.VMEM(observations.shape, f32),
            pltpu.VMEM(obs_weights.shape, f32),
            pltpu.VMEM(damping.shape, f32),
            pltpu.VMEM(transition.shape, f32),
            pltpu.VMEM(obs_matrix.shape, f32),
            pltpu.VMEM((1, width), f32),
            pltpu.SemaphoreType.DMA((6,)),
        ),
        flops=130 * cube,
        limit=32,
        spaces=[pltpu.HBM] * 6,
    )(observations, obs_weights, damping, transition, obs_matrix, prior_row)

    partner = lax.ppermute(total, "tm", swap(count, 1))
    chip, half = call(
        pair_kernel, (struct(rows, width), struct(rows, width // 2)), flops=3 * cube
    )(total, partner)

    straight = [(index, index ^ (4 if index % 2 else 2)) for index in range(count)]
    diagonal = lax.ppermute(half, "tm", swap(count, 6))
    whole = lax.ppermute(chip, "tm", straight)
    middle = width // 2
    power_count = levels + max((count - 1).bit_length(), 1)
    mix, power_high, power_low = call(
        power_kernel,
        (
            struct(2, width, width, dtype=bf16),
            struct(power_count, width, width, dtype=bf16),
            struct(power_count, width, width, dtype=bf16),
        ),
        (
            pltpu.VMEM(transition.shape, f32),
            pltpu.VMEM(transition.shape, f32),
            pltpu.SemaphoreType.DMA((2,)),
        ),
        flops=60 * cube,
        spaces=[pltpu.HBM, pltpu.HBM, pl.ANY],
    )(transition, smoother_gain, half)
    whole, diagonal, mix = lax.optimization_barrier((whole, diagonal, mix))
    halves = jnp.stack([whole[:, :middle], whole[:, middle:], diagonal])
    other_halves = lax.ppermute(halves, "tm", swap(count, 1))
    plane, before, leave = call(
        plane_kernel,
        (struct(rows, width), struct(rows, width), struct(PAD, width)),
        (pltpu.VMEM((4, rows, width), f32), pltpu.VMEM((4, rows, width), f32)),
        flops=9 * cube,
        spaces=[pltpu.VMEM] * 3 + [pl.ANY],
    )(chip, halves, other_halves, mix)
    entry = call(entry_kernel, struct(CHUNKS, rows, width), flops=12 * cube)(
        before, partner, chunk_maps
    )

    enter = jnp.zeros((PAD, width), f32)
    came = came_zero = enter
    hops = count // PLANE - 1
    for hop in range(hops):
        if hop > 0:
            leave, enter = call(
                functools.partial(hop_kernel, hop=hop),
                (struct(PAD, width), struct(PAD, width)),
                flops=cube // 64,
                limit=2,
            )(plane, came, enter)
        low, high = hop * PLANE, (hop + 1) * PLANE
        pairs = [(low + i, high + i) for i in range(1, PLANE, 2)]
        if hop == hops - 1:
            across = [(source, target - 1) for source, target in pairs]
            came_zero = lax.ppermute(leave, "tm", across)
        came = lax.ppermute(leave, "tm", pairs)

    to_zero = [(index, index - 1) for index in range(1, count, 2)]
    enter_zero = lax.ppermute(enter, "tm", to_zero)
    filtered, local = call(
        functools.partial(filter_kernel, levels=levels, hop=hops),
        (struct(steps, width), struct(steps, width)),
        flops=20 * cube,
    )(came, enter, came_zero, enter_zero, entry, path, mix, power_high, power_low)

    sent = jnp.broadcast_to(local[0:1], (count, width))
    offsets = lax.all_to_all(sent, "tm", 0, 0, tiled=True)
    smoothed = call(
        functools.partial(smooth_kernel, levels=levels),
        struct(steps, width),
        (pltpu.VMEM((count + PAD, width), f32),),
        flops=20 * cube,
    )(offsets, local, power_high, power_low)
    return filtered, smoothed


def solution(mesh):
    return jax.shard_map(
        per_device,
        mesh=mesh,
        in_specs=(P("tm", None), P("tm", None), P("tm", None), P(), P(), P(), P()),
        out_specs=(P("tm", None), P("tm", None)),
        check_vma=False,
    )
```

```python
import functools

import jax
import jax.numpy as jnp
from jax import lax
from jax.experimental import pallas as pl
from jax.experimental.pallas import tpu as pltpu
from jax.sharding import PartitionSpec as P

f32, bf16 = jnp.float32, jnp.bfloat16
highest = lax.Precision.HIGHEST
PAD = 8
CHUNKS = 4
PLANE = 8


def exact(left, right):
    return jnp.dot(left, right, precision=highest, preferred_element_type=f32)


def split(value):
    high = value.astype(bf16)
    return high, (value - high.astype(f32)).astype(bf16)


def stack_right(high, low):
    return jnp.concatenate([high, low, high], axis=0)


def dot_split(left, right_stack):
    high, low = split(left)
    return jnp.dot(
        jnp.concatenate([high, high, low], axis=1), right_stack, preferred_element_type=f32
    )


def dot_few(left, right_high, right_low):
    count = left.shape[0]
    high, low = split(left)
    stacked = jnp.concatenate(
        [
            jnp.concatenate([high, high], axis=1),
            jnp.concatenate([low, jnp.zeros_like(low)], axis=1),
        ],
        axis=0,
    )
    right = jnp.concatenate([right_high, right_low], axis=0)
    both = jnp.dot(stacked, right, preferred_element_type=f32)
    return both[:count] + both[count:]


def compose(first, second):
    width = first.shape[1]
    joined = dot_split(first, stack_right(*split(second[:width])))
    return jnp.concatenate([joined[:width], joined[width:] + second[width:]], axis=0)


def eye_map(width):
    rows = lax.broadcasted_iota(jnp.int32, (width + PAD, width), 0)
    cols = lax.broadcasted_iota(jnp.int32, (width + PAD, width), 1)
    return (rows == cols).astype(f32)


def as_column(rows):
    return rows.T[:, 0:1]


def fetch(sources, targets, sems):
    copies = [
        pltpu.make_async_copy(source, target, sems.at[index])
        for index, (source, target) in enumerate(zip(sources, targets))
    ]
    for copy in copies:
        copy.start()
    for copy in copies:
        copy.wait()


def local_kernel(
    obs_hbm, weight_hbm, damp_hbm, trans_hbm, obsmat_hbm, prior_hbm,
    path_ref, chunk_ref, total_ref,
    high_even, low_even, high_odd, low_odd, state_ref, offset_ref, wide_ref, base_ref,
    obs_ref, weight_ref, damp_ref, trans_ref, obsmat_ref, prior_ref, sems,
):
    fetch(
        (trans_hbm, obsmat_hbm, damp_hbm, weight_hbm, obs_hbm, prior_hbm),
        (trans_ref, obsmat_ref, damp_ref, weight_ref, obs_ref, prior_ref),
        sems,
    )
    steps, width = damp_ref.shape
    span = steps // CHUNKS
    is_first = (lax.axis_index("tm") == 0).astype(f32)
    obs_mat = obsmat_ref[...]
    weights = weight_ref[...]
    trans_t = trans_ref[...].T
    base_ref[0] = trans_t
    observed = lax.dot_general(
        trans_t, obs_mat, (((1,), (1,)), ((), ())), precision=highest, preferred_element_type=f32
    )
    base_ref[1] = jnp.concatenate([observed] * 4, axis=1)
    wide_ref[...] = jnp.concatenate([weights] * 4, axis=1)
    obs_high, obs_low = split(obs_mat)
    obs_stack = jnp.concatenate([obs_high, obs_low, obs_high, obs_low], axis=0)

    half = width // 2

    def make(time):
        scaled = base_ref[1] * wide_ref[pl.ds(time, 1), :]
        high, low = split(scaled)
        pieces = jnp.concatenate([high[:, :half], low[:, half:]], axis=1)
        return base_ref[0] - jnp.dot(pieces, obs_stack, preferred_element_type=f32)

    for chunk in range(CHUNKS):
        time = chunk * span
        damp = as_column(jnp.broadcast_to(damp_ref[time : time + 1], (PAD, width)))
        begin = make(time) * damp
        if chunk == 0:
            begin = begin * (1.0 - is_first)
        state_ref[chunk, :width] = begin
        path_ref[time, :width] = begin

    def ready(step, chunk, slot):
        slot[0][chunk], slot[1][chunk] = split(make(chunk * span + step))

    def advance(step, slot, following):
        for chunk in range(CHUNKS):
            time = chunk * span + step
            damped = state_ref[chunk] * damp_ref[pl.ds(time, 1), :]
            moved = dot_split(damped, stack_right(slot[0][chunk], slot[1][chunk]))
            moved = jnp.concatenate(
                [moved[:width], moved[width:] + offset_ref[pl.ds(time, 1), :]], axis=0
            )
            state_ref[chunk] = moved
            path_ref[time] = moved
            if following is not None:
                ready(step + 1, chunk, following)

    even, odd = (high_even, low_even), (high_odd, low_odd)
    for chunk in range(CHUNKS):
        ready(1, chunk, odd)

    offsets = exact(weights * obs_ref[...], obs_mat)
    prior = jnp.broadcast_to(prior_ref[...], (PAD, width))
    seen = lax.dot_general(
        prior, obs_mat, (((1,), (1,)), ((), ())), precision=highest, preferred_element_type=f32
    )
    begun = prior - exact(seen * weights[0:1], obs_mat)
    step_ids = lax.broadcasted_iota(jnp.int32, (steps, 1), 0)
    offsets = offsets + jnp.where(step_ids == 0, is_first, 0.0) * begun[0:1]
    offset_ref[...] = offsets
    for chunk in range(CHUNKS):
        time = chunk * span
        begin = jnp.broadcast_to(offsets[time : time + 1], (PAD, width))
        state_ref[chunk, width:] = begin
        path_ref[time, width:] = begin

    def two(index, carry):
        advance(2 * index + 1, odd, even)
        advance(2 * index + 2, even, odd)
        return carry

    lax.fori_loop(0, span // 2 - 1, two, 0)
    advance(span - 1, odd, None)

    first = compose(state_ref[0], state_ref[1])
    chunk_ref[0] = state_ref[0]
    chunk_ref[1] = first
    chunk_ref[2] = state_ref[2]
    total_ref[...] = compose(first, compose(state_ref[2], state_ref[3]))


def pair_kernel(mine_ref, other_ref, chip_ref, half_ref):
    core = lax.axis_index("tm") % 2
    mine, other = mine_ref[...], other_ref[...]
    upper = core == 1
    whole = compose(jnp.where(upper, other, mine), jnp.where(upper, mine, other))
    chip_ref[...] = whole
    half = whole.shape[1] // 2
    half_ref[...] = jnp.where(upper, whole[:, half:], whole[:, :half])


def plane_kernel(
    chip_ref, mine_ref, other_ref, _, plane_ref, before_ref, leave_ref, all_ref, prefix_ref
):
    me = lax.axis_index("tm")
    upper = me % 2 == 1
    place = (me // 2) % 4
    half = chip_ref.shape[1] // 2
    all_ref[place] = chip_ref[...]
    for part in range(2):
        mine, other = mine_ref[part], other_ref[part]
        columns = pl.ds(part * half, half)
        all_ref[place ^ 1, :, columns] = jnp.where(upper, other, mine)
        all_ref[place ^ 2, :, columns] = jnp.where(upper, mine, other)
    mine, other = mine_ref[2], other_ref[2]
    all_ref[place ^ 3, :, :half] = jnp.where(upper, other, mine)
    all_ref[place ^ 3, :, half:] = jnp.where(upper, mine, other)
    width = chip_ref.shape[1]
    left = compose(all_ref[0], all_ref[1])
    right = compose(all_ref[2], all_ref[3])
    whole = compose(left, right)
    plane_ref[...] = whole
    leave_ref[...] = whole[width:]
    prefix_ref[0] = eye_map(width)
    prefix_ref[1] = all_ref[0]
    prefix_ref[2] = left
    prefix_ref[3] = compose(left, all_ref[2])
    before_ref[...] = prefix_ref[place]


def hop_kernel(plane_ref, came_ref, enter_ref, leave_ref, next_ref, *, hop):
    width = plane_ref.shape[1]
    here = lax.axis_index("tm") // PLANE == hop
    enter = jnp.where(here, came_ref[...], enter_ref[...])
    next_ref[...] = enter
    moved = jnp.sum(plane_ref[:width] * as_column(enter), axis=0, keepdims=True)
    leave_ref[...] = moved + plane_ref[width:]


def entry_kernel(before_ref, other_ref, chunk_ref, entry_ref):
    upper = lax.axis_index("tm") % 2 == 1
    before = before_ref[...]
    joined = compose(before, other_ref[...])
    start = jnp.where(upper, joined, before)
    entry_ref[0] = start
    entry_ref[1] = compose(start, chunk_ref[0])
    entry_ref[2] = compose(start, chunk_ref[1])
    entry_ref[3] = compose(entry_ref[2], chunk_ref[2])


def power_kernel(trans_hbm, gain_hbm, _, mix_ref, high_ref, low_ref, trans_ref, gain_ref, sems):
    fetch((trans_hbm, gain_hbm), (trans_ref, gain_ref), sems)
    gain_t = gain_ref[...].T
    mix_ref[0], mix_ref[1] = split(exact(trans_ref[...].T, gain_t))
    power = gain_t
    for level in range(high_ref.shape[0]):
        high_ref[level], low_ref[level] = split(power)
        if level + 1 < high_ref.shape[0]:
            power = exact(power, power)


def suffix_scan(rows, high_ref, low_ref, first_level, levels):
    count, width = rows.shape
    for level in range(levels):
        distance = 1 << level
        later = jnp.concatenate(
            [rows[distance:], jnp.zeros((distance, width), f32)], axis=0
        )
        rows = rows + dot_few(later, high_ref[first_level + level], low_ref[first_level + level])
    return rows


def filter_kernel(
    came_ref, enter_ref, came_zero_ref, enter_zero_ref, entry_ref, path_ref, mix_ref, high_ref, low_ref,
    filtered_ref, local_ref, *, levels, hop
):
    steps, _, width = path_ref.shape
    span = steps // CHUNKS
    is_final = lax.axis_index("tm") == lax.axis_size("tm") - 1
    me = lax.axis_index("tm")
    here, upper = me // PLANE == hop, me % 2 == 1
    came = jnp.where(upper, came_ref[...], came_zero_ref[...])
    enter = jnp.where(upper, enter_ref[...], enter_zero_ref[...])
    column = as_column(jnp.where(here, came, enter))
    for chunk in range(CHUNKS):
        entry = entry_ref[chunk]
        start = jnp.sum(entry[:width] * column, axis=0, keepdims=True) + entry[width : width + 1]
        begin = as_column(jnp.broadcast_to(start, (PAD, width)))
        for step in range(chunk * span, (chunk + 1) * span):
            path = path_ref[step, :width]
            filtered_ref[step : step + 1] = (
                jnp.sum(path * begin, axis=0, keepdims=True) + path_ref[step, width : width + 1]
            )
    filtered = filtered_ref[...]
    step_ids = lax.broadcasted_iota(jnp.int32, (steps, 1), 0)
    keep = jnp.where(jnp.logical_and(step_ids == steps - 1, is_final), 0.0, 1.0)
    change = filtered - keep * dot_few(filtered, mix_ref[0], mix_ref[1])
    local_ref[...] = suffix_scan(change, high_ref, low_ref, 0, levels)


def smooth_kernel(all_ref, local_ref, high_ref, low_ref, out_ref, sum_ref, *, levels):
    count, width = all_ref.shape
    steps = local_ref.shape[0]
    me = lax.axis_index("tm")
    sum_ref[pl.ds(count, PAD), :] = jnp.zeros((PAD, width), f32)
    sum_ref[pl.ds(0, count), :] = suffix_scan(
        all_ref[...], high_ref, low_ref, levels, (count - 1).bit_length()
    )
    incoming = jnp.broadcast_to(sum_ref[pl.ds(me + 1, 1), :], (PAD, width))
    step_ids = lax.broadcasted_iota(jnp.int32, (steps, 1), 0)
    after = jnp.where(step_ids[:PAD] == 0, incoming, 0.0)
    rows = jnp.concatenate([jnp.zeros((steps, width), f32), after], axis=0)
    lifted = suffix_scan(rows, high_ref, low_ref, 0, levels)[:steps]
    start = sum_ref[pl.ds(me, 1), :]
    out_ref[...] = jnp.where(step_ids == 0, start, local_ref[...] + lifted)


def call(kernel, outs, scratch=(), flops=0, limit=8, spaces=None):
    extra = {} if spaces is None else {"in_specs": [pl.BlockSpec(memory_space=s) for s in spaces]}
    return pl.pallas_call(
        kernel,
        out_shape=outs,
        **extra,
        scratch_shapes=scratch,
        compiler_params=pltpu.CompilerParams(vmem_limit_bytes=limit << 20),
        cost_estimate=pl.CostEstimate(flops=flops, bytes_accessed=1 << 20, transcendentals=0),
    )


def swap(count, distance):
    return [(index, index ^ distance) for index in range(count)]


def per_device(
    observations, obs_weights, damping, transition, obs_matrix, smoother_gain, prior_mean
):
    observations, obs_weights, damping, transition, obs_matrix, smoother_gain, prior_row = (
        pltpu.with_memory_space_constraint(value, pltpu.HBM)
        for value in (
            observations, obs_weights, damping, transition, obs_matrix, smoother_gain,
            prior_mean[None, :],
        )
    )
    steps, width = damping.shape
    count = lax.axis_size("tm")
    rows = width + PAD
    levels = (steps - 1).bit_length()
    cube = 2 * width**3

    def struct(*shape, dtype=f32):
        return jax.ShapeDtypeStruct(shape, dtype)

    path, chunk_maps, total = call(
        local_kernel,
        (struct(steps, rows, width), struct(CHUNKS - 1, rows, width), struct(rows, width)),
        (
            pltpu.VMEM((CHUNKS, width, width), bf16),
            pltpu.VMEM((CHUNKS, width, width), bf16),
            pltpu.VMEM((CHUNKS, width, width), bf16),
            pltpu.VMEM((CHUNKS, width, width), bf16),
            pltpu.VMEM((CHUNKS, rows, width), f32),
            pltpu.VMEM((steps, width), f32),
            pltpu.VMEM((steps, width), f32),
            pltpu.VMEM((2, width, width), f32),
            pltpu.VMEM(observations.shape, f32),
            pltpu.VMEM(obs_weights.shape, f32),
            pltpu.VMEM(damping.shape, f32),
            pltpu.VMEM(transition.shape, f32),
            pltpu.VMEM(obs_matrix.shape, f32),
            pltpu.VMEM((1, width), f32),
            pltpu.SemaphoreType.DMA((6,)),
        ),
        flops=130 * cube,
        limit=32,
        spaces=[pltpu.HBM] * 6,
    )(observations, obs_weights, damping, transition, obs_matrix, prior_row)

    partner = lax.ppermute(total, "tm", swap(count, 1))
    chip, half = call(
        pair_kernel, (struct(rows, width), struct(rows, width // 2)), flops=3 * cube
    )(total, partner)

    straight = [(index, index ^ (4 if index % 2 else 2)) for index in range(count)]
    diagonal = lax.ppermute(half, "tm", swap(count, 6))
    whole = lax.ppermute(chip, "tm", straight)
    middle = width // 2
    power_count = levels + max((count - 1).bit_length(), 1)
    mix, power_high, power_low = call(
        power_kernel,
        (
            struct(2, width, width, dtype=bf16),
            struct(power_count, width, width, dtype=bf16),
            struct(power_count, width, width, dtype=bf16),
        ),
        (
            pltpu.VMEM(transition.shape, f32),
            pltpu.VMEM(transition.shape, f32),
            pltpu.SemaphoreType.DMA((2,)),
        ),
        flops=60 * cube,
        spaces=[pltpu.HBM, pltpu.HBM, pl.ANY],
    )(transition, smoother_gain, half)
    whole, diagonal, mix = lax.optimization_barrier((whole, diagonal, mix))
    halves = jnp.stack([whole[:, :middle], whole[:, middle:], diagonal])
    other_halves = lax.ppermute(halves, "tm", swap(count, 1))
    plane, before, leave = call(
        plane_kernel,
        (struct(rows, width), struct(rows, width), struct(PAD, width)),
        (pltpu.VMEM((4, rows, width), f32), pltpu.VMEM((4, rows, width), f32)),
        flops=9 * cube,
        spaces=[pltpu.VMEM] * 3 + [pl.ANY],
    )(chip, halves, other_halves, mix)
    entry = call(entry_kernel, struct(CHUNKS, rows, width), flops=12 * cube)(
        before, partner, chunk_maps
    )

    enter = jnp.zeros((PAD, width), f32)
    came = came_zero = enter
    hops = count // PLANE - 1
    for hop in range(hops):
        if hop > 0:
            leave, enter = call(
                functools.partial(hop_kernel, hop=hop),
                (struct(PAD, width), struct(PAD, width)),
                flops=cube // 64,
                limit=2,
            )(plane, came, enter)
        low, high = hop * PLANE, (hop + 1) * PLANE
        pairs = [(low + i, high + i) for i in range(1, PLANE, 2)]
        if hop == hops - 1:
            across = [(source, target - 1) for source, target in pairs]
            came_zero = lax.ppermute(leave, "tm", across)
        came = lax.ppermute(leave, "tm", pairs)

    to_zero = [(index, index - 1) for index in range(1, count, 2)]
    enter_zero = lax.ppermute(enter, "tm", to_zero)
    filtered, local = call(
        functools.partial(filter_kernel, levels=levels, hop=hops),
        (struct(steps, width), struct(steps, width)),
        flops=20 * cube,
    )(came, enter, came_zero, enter_zero, entry, path, mix, power_high, power_low)

    sent = jnp.broadcast_to(local[0:1], (count, width))
    offsets = lax.all_to_all(sent, "tm", 0, 0, tiled=True)
    smoothed = call(
        functools.partial(smooth_kernel, levels=levels),
        struct(steps, width),
        (pltpu.VMEM((count + PAD, width), f32),),
        flops=20 * cube,
    )(offsets, local, power_high, power_low)
    return filtered, smoothed


def solution(mesh):
    return jax.shard_map(
        per_device,
        mesh=mesh,
        in_specs=(P("tm", None), P("tm", None), P("tm", None), P(), P(), P(), P()),
        out_specs=(P("tm", None), P("tm", None)),
        check_vma=False,
    )
```
